32 devices in a mesh: beam: 4 (over y, x), row: 4 (over z), col: 2 (over core).
Axes of the slice: x: 2, y: 2, z: 4, core: 2. Of those that a mesh axis runs over, the one named last changes fastest.
Arguments:
- phase_volume: bfloat16 [64, 1024, 256], P('beam', 'row', 'col'), may hold values from -0.75 to 0.75
- absorb_volume: bfloat16 [64, 1024, 256], P('beam', 'row', 'col'), may hold values from -0.375 to 0.375
- probe: float32 [2, 256, 256], replicated, may hold values from -6 to 6
- amplitudes: bfloat16 [4, 2, 32, 256, 256], P('row', 'col', 'beam'), may hold values from 0.19921875 to 2.5
- scan_rows: int32 [4, 2, 32], P('row', 'col', 'beam'), may hold values from 0 to 255
- scan_cols: int32 [4, 2, 32], P('row', 'col', 'beam'), may hold values from 0 to 127
Outputs:
- object_step: float32 [2, 1024, 256], P(None, 'row', 'col')
- probe_gradient: float32 [2, 256, 256], replicated
- loss: float32 [], replicated
The draws below stay inside these ranges and needn't reach their ends.
All inputs are finite; a program needn't handle non-finite values.
Results may differ from the reference program's by a relative error of at most 0.00055.
The reference program's roundings to bfloat16 on the way count: a program that leaves them out, or rounds other values in their place, can miss the bound.
Values sent between devices are 32-bit elements; how exact they have to be, the bound alone decides.
No kernel may reach another device: no remote copies, remote signals or barrier semaphores. Data moves between devices by JAX's collectives and lax.ppermute only.
A program may use at most 64 MiB of HBM per device.

```python
import math
import jax
import jax.numpy as jnp
from jax import lax

ROW_DEV = 256
COL_DEV = 128
PROBE = 256
DEPTH = 64
NROWS = 1024
NCOLS = 256
SCANS = 32
N_ROW = 4
N_COL = 2


def touch_ends(result, stream_key, least, largest):
    longest = result.shape.index(max(result.shape))
    spots = []
    for shift in (0, 1):
        where = [jax.random.randint(jax.random.fold_in(stream_key, axis), (), 0, length) for axis, length in enumerate(result.shape)]
        where[longest] = (where[longest] + shift) % result.shape[longest]
        spots.append(tuple(where))
    return result.at[spots[0]].set(least).at[spots[1]].set(largest)


def block_levels(rng, extent, split, least, largest):
    def one(dim, blocks):
        steps = jax.random.uniform(jax.random.fold_in(jax.random.fold_in(rng, 6), dim), (blocks,), jnp.float32, least / len(split), largest / len(split))
        return jnp.repeat(jnp.exp(steps), extent[dim] // blocks).reshape((-1,) + (1,) * (len(extent) - dim - 1))

    loudness = one(*split[0])
    for cut in split[1:]:
        loudness = loudness * one(*cut)
    return loudness


def normal_values(own_key, shape, scale, most, cuts=(), kind=jnp.bfloat16):
    loudness = block_levels(own_key, shape, cuts, -0.22, 0.18) if cuts else 1.0
    values = jax.random.normal(own_key, shape, jnp.float32) * scale * loudness
    return jnp.minimum(jnp.maximum(values, -most), most).astype(kind)


def setup_inputs(seed: int = 0) -> dict:
    seeds = jax.random.split(jax.random.key(seed), 7)
    return {
        "phase_volume": normal_values(seeds[0], (DEPTH, NROWS, NCOLS), DEPTH ** -0.5, 0.75, ((0, 4), (1, 4), (2, 2))),
        "absorb_volume": normal_values(seeds[1], (DEPTH, NROWS, NCOLS), (4 * DEPTH) ** -0.5, 0.375, ((0, 4), (1, 4), (2, 2))),
        "probe": normal_values(seeds[2], (2, PROBE, PROBE), 1.0, 6.0, (), jnp.float32),
        "amplitudes": jnp.clip(0.19921875 + 2.3007812 * jax.random.uniform(seeds[3], (N_ROW, N_COL, SCANS, PROBE, PROBE), jnp.float32) ** block_levels(seeds[3], (N_ROW, N_COL, SCANS, PROBE, PROBE), ((0, 4), (1, 2), (2, 4)), -0.2, 0.2), 0.19921875, 2.5).astype(jnp.bfloat16),
        "scan_rows": touch_ends(jax.random.randint(seeds[4], (N_ROW, N_COL, SCANS), 0, ROW_DEV), jax.random.fold_in(seeds[4], 1), 0, ROW_DEV - 1).astype(jnp.int32),
        "scan_cols": touch_ends(jax.random.randint(seeds[5], (N_ROW, N_COL, SCANS), 0, COL_DEV), jax.random.fold_in(seeds[5], 1), 0, COL_DEV - 1).astype(jnp.int32),
    }


def dft_tables(length):
    indices = jnp.arange(length, dtype=jnp.int32)
    product = indices[:, None] * indices[None, :] % length
    angles = product.astype(jnp.float32) * (2.0 * math.pi / length)
    factor = 1.0 / math.sqrt(length)
    return ((jnp.cos(angles) * factor).astype(jnp.bfloat16), (-jnp.sin(angles) * factor).astype(jnp.bfloat16))

def left_apply(matrix, batch):
    return jnp.einsum('ab,sbc->sac', matrix.astype(jnp.float32), batch.astype(jnp.float32))

def right_apply(batch, matrix):
    return jnp.einsum('sab,bc->sac', batch.astype(jnp.float32), matrix.astype(jnp.float32))

def window_terms(windows, probe, amplitude, table_real, table_imag):
    phase = windows[:, 0]
    absorb = windows[:, 1]
    damping = jnp.exp(-absorb)
    trans_real = damping * jnp.cos(phase)
    trans_imag = damping * jnp.sin(phase)
    wave_real = probe[0] * trans_real - probe[1] * trans_imag
    wave_imag = probe[0] * trans_imag + probe[1] * trans_real
    send_real = wave_real.astype(jnp.bfloat16)
    send_imag = wave_imag.astype(jnp.bfloat16)
    half_real = (left_apply(table_real, send_real) - left_apply(table_imag, send_imag)).astype(jnp.bfloat16)
    half_imag = (left_apply(table_real, send_imag) + left_apply(table_imag, send_real)).astype(jnp.bfloat16)
    far_real = right_apply(half_real, table_real) - right_apply(half_imag, table_imag)
    far_imag = right_apply(half_real, table_imag) + right_apply(half_imag, table_real)
    modulus = jnp.sqrt(far_real * far_real + far_imag * far_imag)
    misfit = jnp.sum((modulus - amplitude) * (modulus - amplitude))
    ratio = 1.0 - amplitude / jnp.maximum(modulus, 0.5)
    resid_real = (far_real * ratio).astype(jnp.bfloat16)
    resid_imag = (far_imag * ratio).astype(jnp.bfloat16)
    back_real = (left_apply(table_real, resid_real) + left_apply(table_imag, resid_imag)).astype(jnp.bfloat16)
    back_imag = (left_apply(table_real, resid_imag) - left_apply(table_imag, resid_real)).astype(jnp.bfloat16)
    grad_real = right_apply(back_real, table_real) + right_apply(back_imag, table_imag)
    grad_imag = right_apply(back_imag, table_real) - right_apply(back_real, table_imag)
    object_real = wave_real * grad_real + wave_imag * grad_imag
    object_imag = wave_real * grad_imag - wave_imag * grad_real
    cells = jnp.stack([object_imag, -object_real], axis=1)
    probe_real = lax.optimization_barrier(jnp.sum(trans_real * grad_real + trans_imag * grad_imag, axis=0))
    probe_imag = lax.optimization_barrier(jnp.sum(trans_real * grad_imag - trans_imag * grad_real, axis=0))
    return (cells, jnp.stack([probe_real, probe_imag]), misfit)

def reference(phase_volume, absorb_volume, probe, amplitudes, scan_rows, scan_cols):
    half = PROBE // 2
    projection = jnp.stack([lax.optimization_barrier(jnp.sum(phase_volume.astype(jnp.float32), axis=0)), lax.optimization_barrier(jnp.sum(absorb_volume.astype(jnp.float32), axis=0))])
    padded = jnp.pad(projection, ((0, 0), (half, half), (half, half)))
    table_real, table_imag = dft_tables(PROBE)
    tiles = N_ROW * N_COL
    row_list = scan_rows.reshape(tiles, SCANS).astype(jnp.int32)
    col_list = scan_cols.reshape(tiles, SCANS).astype(jnp.int32)
    amp_list = amplitudes.reshape(tiles, SCANS, PROBE, PROBE)
    zero_index = jnp.zeros((), jnp.int32)

    def per_tile(carry, inputs):
        canvas, probe_sum, misfit_sum = carry
        tile, rows_here, cols_here, amp_here = inputs
        row_start = (tile // N_COL * ROW_DEV + rows_here).astype(jnp.int32)
        col_start = (tile % N_COL * COL_DEV + cols_here).astype(jnp.int32)
        windows = jax.vmap(lambda row_at, col_at: lax.dynamic_slice(padded, (zero_index, row_at, col_at), (2, PROBE, PROBE)))(row_start, col_start)
        cells, probe_term, misfit = window_terms(windows, probe, amp_here.astype(jnp.float32), table_real, table_imag)

        def add_window(index, canvas_now):
            where = (zero_index, row_start[index], col_start[index])
            piece = lax.dynamic_slice(canvas_now, where, (2, PROBE, PROBE))
            return lax.dynamic_update_slice(canvas_now, piece + cells[index], where)
        canvas = lax.fori_loop(0, SCANS, add_window, canvas)
        return ((canvas, probe_sum + probe_term, misfit_sum + misfit), None)
    start = (jnp.zeros((2, NROWS + PROBE, NCOLS + PROBE), jnp.float32), jnp.zeros((2, PROBE, PROBE), jnp.float32), jnp.zeros((), jnp.float32))
    inputs = (jnp.arange(tiles, dtype=jnp.int32), row_list, col_list, amp_list)
    (canvas, probe_sum, misfit_sum), _ = lax.scan(per_tile, start, inputs)
    gradient = canvas[:, half:half + NROWS, half:half + NCOLS]
    mean_square = jnp.sum(gradient * gradient) / (2 * NROWS * NCOLS)
    factor = jnp.minimum(1.0, 0.5 / jnp.sqrt(mean_square + 1e-06))
    total = N_ROW * N_COL * SCANS
    return (gradient * factor, probe_sum / total, misfit_sum / (total * PROBE * PROBE))
```

```python
import functools
import math

import jax
import jax.numpy as jnp
import numpy as np
from jax import lax
from jax.experimental import pallas as pl
from jax.experimental.pallas import tpu as pltpu
from jax.sharding import PartitionSpec as P

LANES = 128
SUBS = 8
CHUNK = 32
VMEM = pl.BlockSpec(memory_space=pltpu.VMEM)
SMEM = pl.BlockSpec(memory_space=pltpu.SMEM)
F32 = jnp.float32
BF16 = jnp.bfloat16


def dft_blocks(length):
    indices = np.arange(length, dtype=np.int64)
    product = (indices[:, None] * indices[None, :] % length).astype(np.float32)
    angles = (product * np.float32(2.0 * math.pi / length)).astype(np.float64)
    factor = np.float32(1.0 / math.sqrt(length))
    real = (np.cos(angles).astype(np.float32) * factor).astype(jnp.bfloat16)
    imag = (-np.sin(angles).astype(np.float32) * factor).astype(jnp.bfloat16)
    forward = np.block([[real, -imag], [imag, real]])
    backward = np.block([[real, imag], [-imag, real]])
    return forward.astype(jnp.bfloat16), backward.astype(jnp.bfloat16)


def exchange(value, axis, mask):
    count = lax.axis_size(axis)
    return lax.ppermute(value, axis, [(i, i ^ mask) for i in range(count)])


def rows_of(index, size):
    return pl.ds(pl.multiple_of(index * size, size), size)


def sum_kernel(beams, spot_ref, phase_ref, absorb_ref, *out_refs):
    part = phase_ref.shape[1] // beams
    for k in range(beams):
        where = rows_of(jnp.bitwise_xor(spot_ref[0], k), part)
        for comp, ref in enumerate((phase_ref, absorb_ref)):
            total = ref[0, where, :].astype(F32)
            for d in range(1, ref.shape[0]):
                total = total + ref[d, where, :].astype(F32)
            out_refs[k][comp] = total


def wave_kernel(beams, cols, count, length, *refs):
    spot_ref, row_ref, col_ref = refs[:3]
    mid_refs = refs[3 : 3 + beams]
    left_refs = refs[3 + beams : 3 + 2 * beams]
    right_refs = refs[3 + 2 * beams : 3 + 3 * beams]
    probe_ref, amp_ref, forward_ref, backward_ref = refs[3 + 3 * beams : 7 + 3 * beams]
    sends = 1 if cols == 2 else 2
    outs = refs[7 + 3 * beams : 8 + 3 * beams + sends]
    cells, canvas, probe_sum, miss, trans, psi, half_wave, far, chi, back, near = refs[
        8 + 3 * beams + sends :
    ]
    part = mid_refs[0].shape[1]
    tall = cells.shape[2]
    beam, col = spot_ref[0], spot_ref[2]
    has_left, has_right = col > 0, col < cols - 1
    for k in range(beams):
        quarter = jnp.bitwise_xor(beam, k)
        spots = (quarter + beams // 2, lax.rem(quarter + 3 * beams // 2, 2 * beams))
        for which, at in enumerate(spots):
            where = rows_of(at, part)
            for comp in range(2):
                outside = 1.0 - comp
                source = 2 * which + comp
                cells[comp, 0, where, :] = jnp.where(has_left, left_refs[k][source], outside)
                cells[comp, 1, where, :] = mid_refs[k][source]
                cells[comp, 2, where, :] = jnp.where(has_right, right_refs[k][source], outside)
    canvas[...] = jnp.zeros_like(canvas)
    probe_sum[...] = jnp.zeros_like(probe_sum)
    miss[...] = jnp.zeros_like(miss)
    lane = lax.broadcasted_iota(jnp.int32, (CHUNK, LANES), 1)
    chunks = length // CHUNK

    def window(s, carry):
        row_at, col_at = row_ref[s], col_ref[s]
        back_shift = lax.rem(LANES - col_at, LANES)
        low = lane < LANES - col_at
        for i in range(chunks):
            here = pl.ds(i * CHUNK, CHUNK)
            there = pl.ds(row_at + i * CHUNK, CHUNK)
            pieces = []
            for comp in range(2):
                turned = [
                    pltpu.roll(cells[comp, j, there, :], back_shift, 1) for j in range(3)
                ]
                pieces.append([jnp.where(low, turned[j], turned[j + 1]) for j in range(2)])
            for j in range(2):
                lanes = pl.ds(j * LANES, LANES)
                real, imag = pieces[0][j], pieces[1][j]
                trans[0, j, here, :] = real
                trans[1, j, here, :] = imag
                probe_real = probe_ref[0, here, lanes]
                probe_imag = probe_ref[1, here, lanes]
                psi[here, lanes] = (probe_real * real - probe_imag * imag).astype(BF16)
                psi[pl.ds(length + i * CHUNK, CHUNK), lanes] = (
                    probe_real * imag + probe_imag * real
                ).astype(BF16)
        result = jnp.dot(forward_ref[...], psi[...], preferred_element_type=F32).astype(BF16)
        half_wave[:, :length] = result[:length]
        half_wave[:, length:] = result[length:]
        far[...] = jnp.dot(half_wave[...], backward_ref[...], preferred_element_type=F32)
        for i in range(chunks):
            here = pl.ds(i * CHUNK, CHUNK)
            real, imag = far[here, :length], far[here, length:]
            amplitude = amp_ref[s, here, :].astype(F32)
            power = real * real + imag * imag
            off = jnp.sqrt(power) - amplitude
            wide = off * off
            wide = wide[:, :LANES] + wide[:, LANES:]
            miss[...] += wide.reshape(CHUNK // SUBS, SUBS, LANES).sum(0)
            ratio = 1.0 - amplitude * lax.rsqrt(jnp.maximum(power, 0.25))
            chi[here, :] = (real * ratio).astype(BF16)
            chi[pl.ds(length + i * CHUNK, CHUNK), :] = (imag * ratio).astype(BF16)
        result = jnp.dot(backward_ref[...], chi[...], preferred_element_type=F32).astype(BF16)
        back[:, :length] = result[:length]
        back[:, length:] = result[length:]
        near[...] = jnp.dot(back[...], forward_ref[...], preferred_element_type=F32)
        high = lane >= col_at
        for i in range(chunks):
            here = pl.ds(i * CHUNK, CHUNK)
            there = pl.ds(row_at + i * CHUNK, CHUNK)
            turned = [[], []]
            for j in range(2):
                lanes = pl.ds(j * LANES, LANES)
                grad_real = near[here, lanes]
                grad_imag = near[here, pl.ds(length + j * LANES, LANES)]
                real, imag = trans[0, j, here, :], trans[1, j, here, :]
                probe_sum[0, j, here, :] += real * grad_real + imag * grad_imag
                probe_sum[1, j, here, :] += real * grad_imag - imag * grad_real
                probe_real = probe_ref[0, here, lanes]
                probe_imag = probe_ref[1, here, lanes]
                turned[0].append(
                    pltpu.roll(probe_real * grad_real + probe_imag * grad_imag, col_at, 1)
                )
                turned[1].append(
                    pltpu.roll(probe_real * grad_imag - probe_imag * grad_real, col_at, 1)
                )
            for comp in range(2):
                first, second = turned[comp]
                canvas[comp, 0, there, :] += jnp.where(high, first, 0.0)
                canvas[comp, 1, there, :] += jnp.where(high, second, first)
                canvas[comp, 2, there, :] += jnp.where(high, 0.0, second)
        return carry

    lax.fori_loop(0, count, window, 0)
    base = 2 * tall
    if cols == 2:
        tiles = (1, 2 * has_right.astype(jnp.int32))
        comps = ((col,), (1 - col,))
    else:
        tiles = (1, 0, 2)
        comps = ((0, 1), (), ())
    for out, tile, held in zip(outs, tiles, comps):
        for comp in range(2):
            out[pl.ds(comp * tall, tall), :] = canvas[comp, tile]
        for n, comp in enumerate(held):
            for j in range(2):
                out[pl.ds(base + (2 * n + j) * length, length), :] = probe_sum[comp, j]
        if held:
            out[pl.ds(base + 2 * len(held) * length, SUBS), :] = miss[...]


def split_kernel(beams, tall, length, *refs):
    spot_ref = refs[0]
    ins, outs = refs[1:-beams], refs[-beams:]
    part = tall // (2 * beams)
    strip = length // beams
    planes = (ins[0].shape[0] - 2 * tall - SUBS) // length

    def fetch(where):
        total = ins[0][where, :]
        for ref in ins[1:]:
            total = total + ref[where, :]
        return total

    for k in range(beams):
        quarter = jnp.bitwise_xor(spot_ref[0], k)
        spots = (quarter + beams // 2, lax.rem(quarter + 3 * beams // 2, 2 * beams))
        for which, at in enumerate(spots):
            for comp in range(2):
                where = pl.ds(pl.multiple_of(comp * tall + at * part, SUBS), part)
                outs[k][pl.ds((2 * which + comp) * part, part), :] = fetch(where)
        for n in range(planes):
            start = 2 * tall + n * length + quarter * strip
            where = pl.ds(pl.multiple_of(start, SUBS), strip)
            outs[k][pl.ds(4 * part + n * strip, strip), :] = fetch(where)
        where = pl.ds(2 * tall + planes * length, SUBS)
        outs[k][pl.ds(4 * part + planes * strip, SUBS), :] = fetch(where)


def final_kernel(beams, halves, planes, scale, total, *refs):
    spot_ref = refs[0]
    objects = refs[1 : 1 + beams]
    probes = [refs[1 + (1 + h) * beams : 1 + (2 + h) * beams] for h in range(halves)]
    squares_in = refs[1 + (1 + halves) * beams :][:-3]
    object_ref, probe_ref, loss_ref = refs[-3:]
    part = objects[0].shape[0] // 2
    strip = (probes[0][0].shape[0] - 2 * SUBS) // planes
    length = strip * beams
    miss_at = pl.ds(planes * strip, SUBS)
    square_at = pl.ds(planes * strip + SUBS, SUBS)

    def paired(refs_now, where):
        values = [ref[where, :] for ref in refs_now]
        while len(values) > 1:
            values = [values[i] + values[i + 1] for i in range(0, len(values), 2)]
        return values[0]

    if squares_in:
        squares = squares_in[0][...]
    else:
        squares = paired(probes[0], square_at)
        for more in probes[1:]:
            squares = squares + paired(more, square_at)
    mean_square = jnp.sum(squares, keepdims=True) * scale
    factor = jnp.minimum(1.0, 0.5 / jnp.sqrt(mean_square + 1e-06))
    loss = jnp.sum(probes[0][0][miss_at, :], keepdims=True) / (total * length * length)
    loss_ref[...] = jnp.broadcast_to(loss, loss_ref.shape)
    for k in range(beams):
        quarter = jnp.bitwise_xor(spot_ref[0], k)
        where = rows_of(quarter, part)
        for comp in range(2):
            object_ref[comp, where, :] = objects[k][pl.ds(comp * part, part), :] * factor
        where = rows_of(quarter, strip)
        for h in range(halves):
            for n in range(planes):
                comp = (jnp.bitwise_xor(spot_ref[2], h)) if halves == 2 else n // 2
                lanes = pl.ds((n % 2) * LANES, LANES)
                probe_ref[comp, where, lanes] = (
                    probes[h][k][pl.ds(n * strip, strip), :] * (1.0 / total)
                )


def call(kernel, shapes, scalars, arrays, scratch=(), flops=0):
    size = sum(a.size * a.dtype.itemsize for a in arrays)
    return pl.pallas_call(
        kernel,
        out_shape=[jax.ShapeDtypeStruct(s, F32) for s in shapes],
        in_specs=[SMEM] * len(scalars) + [VMEM] * len(arrays),
        out_specs=[VMEM] * len(shapes),
        scratch_shapes=list(scratch),
        compiler_params=pltpu.CompilerParams(vmem_limit_bytes=40 * 2**20),
        cost_estimate=pl.CostEstimate(flops=flops, bytes_accessed=size, transcendentals=0),
    )(*scalars, *arrays)


def local(phase_volume, absorb_volume, probe, amplitudes, scan_rows, scan_cols):
    length = probe.shape[1]
    count = scan_rows.shape[2]
    rows_local = phase_volume.shape[1]
    cols_local = phase_volume.shape[2]
    beams, rows, cols = (lax.axis_size(a) for a in ("beam", "row", "col"))
    assert cols_local == LANES and length == 2 * LANES and rows_local == length
    beam, row, col = (lax.axis_index(a) for a in ("beam", "row", "col"))
    spot = jnp.stack([beam, row, col]).astype(jnp.int32)
    part = rows_local // beams
    tall = rows_local + length
    others = range(1, beams)
    near_half = beams // 2

    def toward(step):
        pairs = []
        for b in range(beams):
            way = step if b >= near_half else -step
            for r in range(rows):
                if 0 <= r + way < rows:
                    pairs.append((b * rows + r, b * rows + r + way))
        return pairs

    sums = call(
        functools.partial(sum_kernel, beams),
        [(2, part, LANES)] * beams,
        [spot],
        [phase_volume, absorb_volume],
    )
    got = [sums[0]] + [exchange(sums[k], "beam", k) for k in others]
    total = functools.reduce(jnp.add, got)
    damping = jnp.exp(-total[1])
    trans = jnp.stack([damping * jnp.cos(total[0]), damping * jnp.sin(total[0])])
    halo = lax.ppermute(trans, ("beam", "row"), toward(1))
    inside = jnp.where(beam >= near_half, row > 0, row < rows - 1)
    outside = jnp.arange(2, dtype=jnp.int32).reshape(2, 1, 1) == 0
    halo = jnp.where(inside, halo, jnp.where(outside, 1.0, 0.0))
    own = jnp.concatenate([trans, halo])
    mids = [own] + [exchange(own, "beam", k) for k in others]
    if cols == 2:
        lefts = [exchange(x, "col", 1) for x in mids]
        rights = lefts
    else:
        lefts = [lax.ppermute(x, "col", [(i, i + 1) for i in range(cols - 1)]) for x in mids]
        rights = [lax.ppermute(x, "col", [(i + 1, i) for i in range(cols - 1)]) for x in mids]
    forward, backward = dft_blocks(length)
    paired = cols == 2
    planes = 2 if paired else 4
    deep = 2 * tall + planes * length + SUBS
    shapes = [(deep, LANES)] * 2 if paired else [(deep, LANES)] + [(2 * tall, LANES)] * 2
    outs = call(
        functools.partial(wave_kernel, beams, cols, count, length),
        shapes,
        [spot, scan_rows.reshape(count), scan_cols.reshape(count)],
        [*mids, *lefts, *rights, probe, amplitudes.reshape(count, length, length)]
        + [jnp.asarray(forward), jnp.asarray(backward)],
        [
            pltpu.VMEM((2, 3, tall, LANES), F32),
            pltpu.VMEM((2, 3, tall, LANES), F32),
            pltpu.VMEM((2, 2, length, LANES), F32),
            pltpu.VMEM((SUBS, LANES), F32),
            pltpu.VMEM((2, 2, length, LANES), F32),
            pltpu.VMEM((2 * length, length), BF16),
            pltpu.VMEM((length, 2 * length), BF16),
            pltpu.VMEM((length, 2 * length), F32),
            pltpu.VMEM((2 * length, length), BF16),
            pltpu.VMEM((length, 2 * length), BF16),
            pltpu.VMEM((length, 2 * length), F32),
        ],
        flops=count * 32 * length**3,
    )
    if paired:
        pieces = [outs[0], exchange(outs[1], "col", 1)]
    else:
        keep, to_left, to_right = outs
        edge = lax.ppermute(to_left, "col", [(i + 1, i) for i in range(cols - 1)])
        edge = edge + lax.ppermute(to_right, "col", [(i, i + 1) for i in range(cols - 1)])
        rest = lax.psum(keep[2 * tall :], "col")
        pieces = [jnp.concatenate([keep[: 2 * tall] + edge, rest])]
    strip = length // beams
    flat = 4 * part + planes * strip + SUBS
    split = call(
        functools.partial(split_kernel, beams, tall, length),
        [(flat, LANES)] * beams,
        [spot],
        pieces,
    )

    def butterfly(values):
        while len(values) > 1:
            values = [values[i] + values[i + 1] for i in range(0, len(values), 2)]
        return values[0]

    got = [split[0]] + [exchange(split[k], "beam", k) for k in others]
    summed = butterfly(got)
    halo = lax.ppermute(summed[2 * part : 4 * part], ("beam", "row"), toward(-1))
    whole = summed[: 2 * part] + halo
    real, imag = whole[:part], whole[part:]
    grad_phase = trans[0] * imag - trans[1] * real
    grad_absorb = -(trans[0] * real + trans[1] * imag)
    squares = grad_phase * grad_phase + grad_absorb * grad_absorb
    squares = squares.reshape(part // SUBS, SUBS, LANES).sum(0)
    gradient = jnp.concatenate([grad_phase, grad_absorb])
    objects = [gradient] + [exchange(gradient, "beam", k) for k in others]
    carried = jnp.concatenate([summed[4 * part :], squares])
    carried = butterfly([carried] + [exchange(carried, "row", k) for k in range(1, rows)])
    probes = [carried] + [exchange(carried, "beam", k) for k in others]
    operands = objects + probes
    if paired:
        operands = operands + [exchange(x, "col", 1) for x in probes]
    else:
        at = planes * strip + SUBS
        operands = operands + [lax.psum(butterfly([x[at:] for x in probes]), "col")]
    plane_devices = rows * cols
    objects_step, probe_gradient, loss = call(
        functools.partial(
            final_kernel,
            beams,
            2 if paired else 1,
            planes,
            1.0 / (2 * rows_local * cols_local * plane_devices),
            float(plane_devices * beams * count),
        ),
        [(2, rows_local, cols_local), (2, length, length), (1, 1)],
        [spot],
        operands,
    )
    return objects_step, probe_gradient, loss[0, 0]


def solution(mesh):
    in_specs = (
        P("beam", "row", "col"),
        P("beam", "row", "col"),
        P(),
        P("row", "col", "beam", None, None),
        P("row", "col", "beam"),
        P("row", "col", "beam"),
    )
    out_specs = (P(None, "row", "col"), P(), P())
    return jax.shard_map(local, mesh=mesh, in_specs=in_specs, out_specs=out_specs, check_vma=False)
```

```python
import functools
import math

import jax
import jax.numpy as jnp
import numpy as np
from jax import lax
from jax.experimental import pallas as pl
from jax.experimental.pallas import tpu as pltpu
from jax.sharding import PartitionSpec as P

LANES = 128
SUBS = 8
CHUNK = 32
TOGETHER = 4
VMEM = pl.BlockSpec(memory_space=pltpu.VMEM)
SMEM = pl.BlockSpec(memory_space=pltpu.SMEM)
F32 = jnp.float32
BF16 = jnp.bfloat16


def dft_blocks(length):
    indices = np.arange(length, dtype=np.int64)
    product = (indices[:, None] * indices[None, :] % length).astype(np.float32)
    angles = (product * np.float32(2.0 * math.pi / length)).astype(np.float64)
    factor = np.float32(1.0 / math.sqrt(length))
    real = (np.cos(angles).astype(np.float32) * factor).astype(jnp.bfloat16)
    imag = (-np.sin(angles).astype(np.float32) * factor).astype(jnp.bfloat16)
    forward = np.block([[real, -imag], [imag, real]])
    backward = np.block([[real, imag], [-imag, real]])
    return forward.astype(jnp.bfloat16), backward.astype(jnp.bfloat16)


def exchange(value, axis, mask):
    count = lax.axis_size(axis)
    return lax.ppermute(value, axis, [(i, i ^ mask) for i in range(count)])


def rows_of(index, size):
    return pl.ds(pl.multiple_of(index * size, size), size)


def sum_kernel(beams, spot_ref, phase_ref, absorb_ref, *out_refs):
    part = phase_ref.shape[1] // beams
    for k in range(beams):
        where = rows_of(jnp.bitwise_xor(spot_ref[0], k), part)
        for comp, ref in enumerate((phase_ref, absorb_ref)):
            total = ref[0, where, :].astype(F32)
            for d in range(1, ref.shape[0]):
                total = total + ref[d, where, :].astype(F32)
            out_refs[k][comp] = total


def wave_kernel(beams, cols, count, length, *refs):
    spot_ref, row_ref, col_ref = refs[:3]
    mid_refs = refs[3 : 3 + beams]
    left_refs = refs[3 + beams : 3 + 2 * beams]
    right_refs = refs[3 + 2 * beams : 3 + 3 * beams]
    probe_ref, amp_ref, forward_ref, backward_ref = refs[3 + 3 * beams : 7 + 3 * beams]
    sends = 1 if cols == 2 else 2
    outs = refs[7 + 3 * beams : 8 + 3 * beams + sends]
    cells, canvas, probe_sum, miss, trans, psi, half_wave, far, chi, back, near = refs[
        8 + 3 * beams + sends :
    ]
    part = mid_refs[0].shape[1]
    tall = cells.shape[2]
    together = trans.shape[0]
    beam, col = spot_ref[0], spot_ref[2]
    has_left, has_right = col > 0, col < cols - 1
    for k in range(beams):
        quarter = jnp.bitwise_xor(beam, k)
        spots = (quarter + beams // 2, lax.rem(quarter + 3 * beams // 2, 2 * beams))
        for which, at in enumerate(spots):
            where = rows_of(at, part)
            for comp in range(2):
                outside = 1.0 - comp
                source = 2 * which + comp
                cells[comp, 0, where, :] = jnp.where(has_left, left_refs[k][source], outside)
                cells[comp, 1, where, :] = mid_refs[k][source]
                cells[comp, 2, where, :] = jnp.where(has_right, right_refs[k][source], outside)
    canvas[...] = jnp.zeros_like(canvas)
    probe_sum[...] = jnp.zeros_like(probe_sum)
    miss[...] = jnp.zeros_like(miss)
    lane = lax.broadcasted_iota(jnp.int32, (CHUNK, LANES), 1)
    chunks = length // CHUNK

    def make_psi(s, u):
        row_at, col_at = row_ref[s], col_ref[s]
        back_shift = lax.rem(LANES - col_at, LANES)
        low = lane < LANES - col_at
        for i in range(chunks):
            here = pl.ds(i * CHUNK, CHUNK)
            there = pl.ds(row_at + i * CHUNK, CHUNK)
            pieces = []
            for comp in range(2):
                turned = [
                    pltpu.roll(cells[comp, j, there, :], back_shift, 1) for j in range(3)
                ]
                pieces.append([jnp.where(low, turned[j], turned[j + 1]) for j in range(2)])
            for j in range(2):
                lanes = pl.ds(j * LANES, LANES)
                real, imag = pieces[0][j], pieces[1][j]
                trans[u, 0, j, here, :] = real
                trans[u, 1, j, here, :] = imag
                probe_real = probe_ref[0, here, lanes]
                probe_imag = probe_ref[1, here, lanes]
                psi[u, here, lanes] = (probe_real * real - probe_imag * imag).astype(BF16)
                psi[u, pl.ds(length + i * CHUNK, CHUNK), lanes] = (
                    probe_real * imag + probe_imag * real
                ).astype(BF16)

    def left_product(table, source, target, u):
        result = jnp.dot(table[...], source[u], preferred_element_type=F32).astype(BF16)
        target[u, :, :length] = result[:length]
        target[u, :, length:] = result[length:]

    def right_product(source, table, target, u):
        target[u] = jnp.dot(source[u], table[...], preferred_element_type=F32)

    def make_chi(s, u):
        for i in range(chunks):
            here = pl.ds(i * CHUNK, CHUNK)
            real, imag = far[u, here, :length], far[u, here, length:]
            amplitude = amp_ref[s, here, :].astype(F32)
            power = real * real + imag * imag
            off = jnp.sqrt(power) - amplitude
            wide = off * off
            wide = wide[:, :LANES] + wide[:, LANES:]
            miss[...] += wide.reshape(CHUNK // SUBS, SUBS, LANES).sum(0)
            ratio = 1.0 - amplitude * lax.rsqrt(jnp.maximum(power, 0.25))
            chi[u, here, :] = (real * ratio).astype(BF16)
            chi[u, pl.ds(length + i * CHUNK, CHUNK), :] = (imag * ratio).astype(BF16)

    def scatter(s, u):
        row_at, col_at = row_ref[s], col_ref[s]
        high = lane >= col_at
        for i in range(chunks):
            here = pl.ds(i * CHUNK, CHUNK)
            there = pl.ds(row_at + i * CHUNK, CHUNK)
            turned = [[], []]
            for j in range(2):
                lanes = pl.ds(j * LANES, LANES)
                grad_real = near[u, here, lanes]
                grad_imag = near[u, here, pl.ds(length + j * LANES, LANES)]
                real, imag = trans[u, 0, j, here, :], trans[u, 1, j, here, :]
                probe_sum[0, j, here, :] += real * grad_real + imag * grad_imag
                probe_sum[1, j, here, :] += real * grad_imag - imag * grad_real
                probe_real = probe_ref[0, here, lanes]
                probe_imag = probe_ref[1, here, lanes]
                turned[0].append(
                    pltpu.roll(probe_real * grad_real + probe_imag * grad_imag, col_at, 1)
                )
                turned[1].append(
                    pltpu.roll(probe_real * grad_imag - probe_imag * grad_real, col_at, 1)
                )
            for comp in range(2):
                first, second = turned[comp]
                canvas[comp, 0, there, :] += jnp.where(high, first, 0.0)
                canvas[comp, 1, there, :] += jnp.where(high, second, first)
                canvas[comp, 2, there, :] += jnp.where(high, 0.0, second)

    def group(g, carry):
        for u in range(together):
            make_psi(g * together + u, u)
            left_product(forward_ref, psi, half_wave, u)
        for u in range(together):
            right_product(half_wave, backward_ref, far, u)
        for u in range(together):
            make_chi(g * together + u, u)
            left_product(backward_ref, chi, back, u)
        for u in range(together):
            right_product(back, forward_ref, near, u)
        for u in range(together):
            scatter(g * together + u, u)
        return carry

    lax.fori_loop(0, count // together, group, 0)
    base = 2 * tall
    if cols == 2:
        tiles = (1, 2 * has_right.astype(jnp.int32))
        comps = ((col,), (1 - col,))
    else:
        tiles = (1, 0, 2)
        comps = ((0, 1), (), ())
    for out, tile, held in zip(outs, tiles, comps):
        for comp in range(2):
            out[pl.ds(comp * tall, tall), :] = canvas[comp, tile]
        for n, comp in enumerate(held):
            for j in range(2):
                out[pl.ds(base + (2 * n + j) * length, length), :] = probe_sum[comp, j]
        if held:
            out[pl.ds(base + 2 * len(held) * length, SUBS), :] = miss[...]


def split_kernel(beams, tall, length, *refs):
    spot_ref = refs[0]
    ins, outs, edges = refs[1 : -2 * beams], refs[-2 * beams : -beams], refs[-beams:]
    part = tall // (2 * beams)
    strip = length // beams
    planes = (ins[0].shape[0] - 2 * tall - SUBS) // length

    def fetch(where):
        total = ins[0][where, :]
        for ref in ins[1:]:
            total = total + ref[where, :]
        return total

    for k in range(beams):
        quarter = jnp.bitwise_xor(spot_ref[0], k)
        spots = (quarter + beams // 2, lax.rem(quarter + 3 * beams // 2, 2 * beams))
        for out, at in zip((outs[k], edges[k]), spots):
            for comp in range(2):
                where = pl.ds(pl.multiple_of(comp * tall + at * part, SUBS), part)
                out[pl.ds(comp * part, part), :] = fetch(where)
        for n in range(planes):
            start = 2 * tall + n * length + quarter * strip
            where = pl.ds(pl.multiple_of(start, SUBS), strip)
            outs[k][pl.ds(2 * part + n * strip, strip), :] = fetch(where)
        where = pl.ds(2 * tall + planes * length, SUBS)
        outs[k][pl.ds(2 * part + planes * strip, SUBS), :] = fetch(where)


def final_kernel(beams, halves, planes, scale, total, *refs):
    spot_ref = refs[0]
    objects = refs[1 : 1 + beams]
    probes = [refs[1 + (1 + h) * beams : 1 + (2 + h) * beams] for h in range(halves)]
    squares_in = refs[1 + (1 + halves) * beams :][:-3]
    object_ref, probe_ref, loss_ref = refs[-3:]
    part = objects[0].shape[0] // 2
    strip = (probes[0][0].shape[0] - 2 * SUBS) // planes
    length = strip * beams
    miss_at = pl.ds(planes * strip, SUBS)
    square_at = pl.ds(planes * strip + SUBS, SUBS)

    def paired(refs_now, where):
        values = [ref[where, :] for ref in refs_now]
        while len(values) > 1:
            values = [values[i] + values[i + 1] for i in range(0, len(values), 2)]
        return values[0]

    if squares_in:
        squares = squares_in[0][...]
    else:
        squares = paired(probes[0], square_at)
        for more in probes[1:]:
            squares = squares + paired(more, square_at)
    mean_square = jnp.sum(squares, keepdims=True) * scale
    factor = jnp.minimum(1.0, 0.5 / jnp.sqrt(mean_square + 1e-06))
    loss = jnp.sum(probes[0][0][miss_at, :], keepdims=True) / (total * length * length)
    loss_ref[...] = jnp.broadcast_to(loss, loss_ref.shape)
    for k in range(beams):
        quarter = jnp.bitwise_xor(spot_ref[0], k)
        where = rows_of(quarter, part)
        for comp in range(2):
            object_ref[comp, where, :] = objects[k][pl.ds(comp * part, part), :] * factor
        where = rows_of(quarter, strip)
        for h in range(halves):
            for n in range(planes):
                comp = (jnp.bitwise_xor(spot_ref[2], h)) if halves == 2 else n // 2
                lanes = pl.ds((n % 2) * LANES, LANES)
                probe_ref[comp, where, lanes] = (
                    probes[h][k][pl.ds(n * strip, strip), :] * (1.0 / total)
                )


def call(kernel, shapes, scalars, arrays, scratch=(), flops=0):
    size = sum(a.size * a.dtype.itemsize for a in arrays)
    return pl.pallas_call(
        kernel,
        out_shape=[jax.ShapeDtypeStruct(s, F32) for s in shapes],
        in_specs=[SMEM] * len(scalars) + [VMEM] * len(arrays),
        out_specs=[VMEM] * len(shapes),
        scratch_shapes=list(scratch),
        compiler_params=pltpu.CompilerParams(vmem_limit_bytes=40 * 2**20),
        cost_estimate=pl.CostEstimate(flops=flops, bytes_accessed=size, transcendentals=0),
    )(*scalars, *arrays)


def wave_call(sizes, scalars, arrays):
    beams, cols, count, length, tall = sizes
    paired = cols == 2
    deep = 2 * tall + (2 if paired else 4) * length + SUBS
    shapes = [(deep, LANES)] * 2 if paired else [(deep, LANES)] + [(2 * tall, LANES)] * 2
    u = math.gcd(count, TOGETHER)
    return call(
        functools.partial(wave_kernel, beams, cols, count, length),
        shapes,
        scalars,
        arrays + [jnp.asarray(table) for table in dft_blocks(length)],
        [
            pltpu.VMEM((2, 3, tall, LANES), F32),
            pltpu.VMEM((2, 3, tall, LANES), F32),
            pltpu.VMEM((2, 2, length, LANES), F32),
            pltpu.VMEM((SUBS, LANES), F32),
            pltpu.VMEM((u, 2, 2, length, LANES), F32),
            pltpu.VMEM((u, 2 * length, length), BF16),
            pltpu.VMEM((u, length, 2 * length), BF16),
            pltpu.VMEM((u, length, 2 * length), F32),
            pltpu.VMEM((u, 2 * length, length), BF16),
            pltpu.VMEM((u, length, 2 * length), BF16),
            pltpu.VMEM((u, length, 2 * length), F32),
        ],
        flops=count * 32 * length**3,
    )


def local(phase_volume, absorb_volume, probe, amplitudes, scan_rows, scan_cols):
    length = probe.shape[1]
    count = scan_rows.shape[2]
    rows_local = phase_volume.shape[1]
    cols_local = phase_volume.shape[2]
    beams, rows, cols = (lax.axis_size(a) for a in ("beam", "row", "col"))
    assert cols_local == LANES and length == 2 * LANES and rows_local == length
    beam, row, col = (lax.axis_index(a) for a in ("beam", "row", "col"))
    spot = jnp.stack([beam, row, col]).astype(jnp.int32)
    part = rows_local // beams
    tall = rows_local + length
    others = range(1, beams)
    near_half = beams // 2

    def toward(value, k, step):
        pairs = []
        for b in range(beams):
            way = step if b ^ k >= near_half else -step
            for r in range(rows):
                if 0 <= r + way < rows:
                    pairs.append((b * rows + r, (b ^ k) * rows + r + way))
        return lax.ppermute(value, ("beam", "row"), pairs)

    sums = call(
        functools.partial(sum_kernel, beams),
        [(2, part, LANES)] * beams,
        [spot],
        [phase_volume, absorb_volume],
    )
    edges = [toward(sums[k], k, 1) for k in range(beams)]
    got = [sums[0]] + [exchange(sums[k], "beam", k) for k in others]
    total = jnp.stack([functools.reduce(jnp.add, got), functools.reduce(jnp.add, edges)])
    damping = jnp.exp(-total[:, 1])
    own = jnp.stack([damping * jnp.cos(total[:, 0]), damping * jnp.sin(total[:, 0])], axis=1)
    trans = own[0]
    own = own.reshape(4, part, LANES)
    mids = [own] + [exchange(own, "beam", k) for k in others]
    if cols == 2:
        lefts = [exchange(x, "col", 1) for x in mids]
        rights = lefts
    else:
        lefts = [lax.ppermute(x, "col", [(i, i + 1) for i in range(cols - 1)]) for x in mids]
        rights = [lax.ppermute(x, "col", [(i + 1, i) for i in range(cols - 1)]) for x in mids]
    paired = cols == 2
    planes = 2 if paired else 4
    outs = wave_call(
        (beams, cols, count, length, tall),
        [spot, scan_rows.reshape(count), scan_cols.reshape(count)],
        [*mids, *lefts, *rights, probe, amplitudes.reshape(count, length, length)],
    )
    if paired:
        pieces = [outs[0], exchange(outs[1], "col", 1)]
    else:
        keep, to_left, to_right = outs
        edge = lax.ppermute(to_left, "col", [(i + 1, i) for i in range(cols - 1)])
        edge = edge + lax.ppermute(to_right, "col", [(i, i + 1) for i in range(cols - 1)])
        rest = lax.psum(keep[2 * tall :], "col")
        pieces = [jnp.concatenate([keep[: 2 * tall] + edge, rest])]
    strip = length // beams
    flat = 2 * part + planes * strip + SUBS
    split = call(
        functools.partial(split_kernel, beams, tall, length),
        [(flat, LANES)] * beams + [(2 * part, LANES)] * beams,
        [spot],
        pieces,
    )

    def butterfly(values):
        while len(values) > 1:
            values = [values[i] + values[i + 1] for i in range(0, len(values), 2)]
        return values[0]

    edges = [toward(split[beams + k], k, -1) for k in range(beams)]
    got = [split[0]] + [exchange(split[k], "beam", k) for k in others]
    summed = butterfly(got)
    whole = summed[: 2 * part] + butterfly(edges)
    real, imag = whole[:part], whole[part:]
    grad_phase = trans[0] * imag - trans[1] * real
    grad_absorb = -(trans[0] * real + trans[1] * imag)
    squares = grad_phase * grad_phase + grad_absorb * grad_absorb
    squares = squares.reshape(part // SUBS, SUBS, LANES).sum(0)
    gradient = jnp.concatenate([grad_phase, grad_absorb])
    carried = jnp.concatenate([summed[2 * part :], squares])
    from_rows = [exchange(carried, "row", k) for k in range(1, rows)]
    objects = [gradient] + [exchange(gradient, "beam", k) for k in others]
    carried = butterfly([carried] + from_rows)
    probes = [carried] + [exchange(carried, "beam", k) for k in others]
    operands = objects + probes
    if paired:
        operands = operands + [exchange(x, "col", 1) for x in probes]
    else:
        at = planes * strip + SUBS
        operands = operands + [lax.psum(butterfly([x[at:] for x in probes]), "col")]
    plane_devices = rows * cols
    objects_step, probe_gradient, loss = call(
        functools.partial(
            final_kernel,
            beams,
            2 if paired else 1,
            planes,
            1.0 / (2 * rows_local * cols_local * plane_devices),
            float(plane_devices * beams * count),
        ),
        [(2, rows_local, cols_local), (2, length, length), (1, 1)],
        [spot],
        operands,
    )
    return objects_step, probe_gradient, loss[0, 0]


def solution(mesh):
    in_specs = (
        P("beam", "row", "col"),
        P("beam", "row", "col"),
        P(),
        P("row", "col", "beam", None, None),
        P("row", "col", "beam"),
        P("row", "col", "beam"),
    )
    out_specs = (P(None, "row", "col"), P(), P())
    return jax.shard_map(local, mesh=mesh, in_specs=in_specs, out_specs=out_specs, check_vma=False)
```

```python
import functools
import math

import jax
import jax.numpy as jnp
import numpy as np
from jax import lax
from jax.experimental import pallas as pl
from jax.experimental.pallas import tpu as pltpu
from jax.sharding import PartitionSpec as P

LANES = 128
SUBS = 8
CHUNK = 32
TOGETHER = 8
VMEM = pl.BlockSpec(memory_space=pltpu.VMEM)
SMEM = pl.BlockSpec(memory_space=pltpu.SMEM)
HBM = pl.BlockSpec(memory_space=pltpu.HBM)
F32 = jnp.float32
BF16 = jnp.bfloat16


def dft_blocks(length):
    indices = np.arange(length, dtype=np.int64)
    product = (indices[:, None] * indices[None, :] % length).astype(np.float32)
    angles = (product * np.float32(2.0 * math.pi / length)).astype(np.float64)
    factor = np.float32(1.0 / math.sqrt(length))
    real = (np.cos(angles).astype(np.float32) * factor).astype(jnp.bfloat16)
    imag = (-np.sin(angles).astype(np.float32) * factor).astype(jnp.bfloat16)
    forward = np.block([[real, -imag], [imag, real]])
    backward = np.block([[real, imag], [-imag, real]])
    return forward.astype(jnp.bfloat16), backward.astype(jnp.bfloat16)


def exchange(value, axis, mask):
    count = lax.axis_size(axis)
    return lax.ppermute(value, axis, [(i, i ^ mask) for i in range(count)])


def butterfly(values):
    while len(values) > 1:
        values = [values[i] + values[i + 1] for i in range(0, len(values), 2)]
    return values[0]


def rows_of(index, size):
    return pl.ds(pl.multiple_of(index * size, size), size)


def sum_kernel(beams, spot_ref, phase_ref, absorb_ref, *refs):
    outs, (phase_now, absorb_now, sums, sems) = refs[:beams], refs[beams:]
    part = phase_now.shape[1] // beams
    copies = []
    for q in range(beams):
        where = pl.ds(q * part, part)
        for comp, (a, b) in enumerate(((phase_ref, phase_now), (absorb_ref, absorb_now))):
            copy = pltpu.make_async_copy(
                a.at[:, where, :], b.at[:, where, :], sems.at[2 * q + comp]
            )
            copy.start()
            copies.append(copy)
    for q in range(beams):
        where = pl.ds(q * part, part)
        for comp, ref in enumerate((phase_now, absorb_now)):
            copies[2 * q + comp].wait()
            total = ref[0, where, :].astype(F32)
            for d in range(1, ref.shape[0]):
                total = total + ref[d, where, :].astype(F32)
            sums[q, comp] = total
    for k in range(beams):
        outs[k][...] = sums[jnp.bitwise_xor(spot_ref[0], k)]


def wave_kernel(beams, cols, count, length, *refs):
    spot_ref = refs[0]
    mid_refs = refs[1 : 1 + beams]
    left_refs = refs[1 + beams : 1 + 2 * beams]
    right_refs = refs[1 + 2 * beams : 1 + 3 * beams]
    probe_ref, amp_ref, forward_ref, backward_ref = refs[1 + 3 * beams : 5 + 3 * beams]
    sends = 1 if cols == 2 else 2
    outs = refs[5 + 3 * beams : 6 + 3 * beams + sends]
    cells, canvas, probe_sum, miss, trans, psi, half_wave, far, chi, back, near = refs[
        6 + 3 * beams + sends :
    ]
    part = mid_refs[0].shape[1]
    tall = cells.shape[2]
    together = trans.shape[0]
    beam, col = spot_ref[0], spot_ref[2]
    has_left, has_right = col > 0, col < cols - 1
    for k in range(beams):
        quarter = jnp.bitwise_xor(beam, k)
        spots = (quarter + beams // 2, lax.rem(quarter + 3 * beams // 2, 2 * beams))
        for which, at in enumerate(spots):
            where = rows_of(at, part)
            for comp in range(2):
                outside = 1.0 - comp
                source = 2 * which + comp
                cells[comp, 0, where, :] = jnp.where(has_left, left_refs[k][source], outside)
                cells[comp, 1, where, :] = mid_refs[k][source]
                cells[comp, 2, where, :] = jnp.where(has_right, right_refs[k][source], outside)
    canvas[...] = jnp.zeros_like(canvas)
    probe_sum[...] = jnp.zeros_like(probe_sum)
    miss[...] = jnp.zeros_like(miss)
    lane = lax.broadcasted_iota(jnp.int32, (CHUNK, LANES), 1)
    chunks = length // CHUNK

    def make_psi(s, u):
        row_at, col_at = spot_ref[3 + s], spot_ref[3 + count + s]
        back_shift = lax.rem(LANES - col_at, LANES)
        low = lane < LANES - col_at
        for i in range(chunks):
            here = pl.ds(i * CHUNK, CHUNK)
            there = pl.ds(row_at + i * CHUNK, CHUNK)
            pieces = []
            for comp in range(2):
                turned = [
                    pltpu.roll(cells[comp, j, there, :], back_shift, 1) for j in range(3)
                ]
                pieces.append([jnp.where(low, turned[j], turned[j + 1]) for j in range(2)])
            for j in range(2):
                lanes = pl.ds(j * LANES, LANES)
                real, imag = pieces[0][j], pieces[1][j]
                trans[u, 0, j, here, :] = real
                trans[u, 1, j, here, :] = imag
                probe_real = probe_ref[0, here, lanes]
                probe_imag = probe_ref[1, here, lanes]
                psi[u, here, lanes] = (probe_real * real - probe_imag * imag).astype(BF16)
                psi[u, pl.ds(length + i * CHUNK, CHUNK), lanes] = (
                    probe_real * imag + probe_imag * real
                ).astype(BF16)

    def left_product(table, source, target, u):
        result = jnp.dot(table[...], source[u], preferred_element_type=F32).astype(BF16)
        target[u, :, :length] = result[:length]
        target[u, :, length:] = result[length:]

    def right_product(source, table, target, u):
        target[u] = jnp.dot(source[u], table[...], preferred_element_type=F32)

    def make_chi(s, u):
        for i in range(chunks):
            here = pl.ds(i * CHUNK, CHUNK)
            real, imag = far[u, here, :length], far[u, here, length:]
            amplitude = amp_ref[s, here, :].astype(F32)
            power = real * real + imag * imag
            off = jnp.sqrt(power) - amplitude
            wide = off * off
            wide = wide[:, :LANES] + wide[:, LANES:]
            miss[...] += wide.reshape(CHUNK // SUBS, SUBS, LANES).sum(0)
            ratio = 1.0 - amplitude * lax.rsqrt(jnp.maximum(power, 0.25))
            chi[u, here, :] = (real * ratio).astype(BF16)
            chi[u, pl.ds(length + i * CHUNK, CHUNK), :] = (imag * ratio).astype(BF16)

    def scatter(s, u):
        row_at, col_at = spot_ref[3 + s], spot_ref[3 + count + s]
        high = lane >= col_at
        for i in range(chunks):
            here = pl.ds(i * CHUNK, CHUNK)
            there = pl.ds(row_at + i * CHUNK, CHUNK)
            turned = [[], []]
            for j in range(2):
                lanes = pl.ds(j * LANES, LANES)
                grad_real = near[u, here, lanes]
                grad_imag = near[u, here, pl.ds(length + j * LANES, LANES)]
                real, imag = trans[u, 0, j, here, :], trans[u, 1, j, here, :]
                probe_sum[0, j, here, :] += real * grad_real + imag * grad_imag
                probe_sum[1, j, here, :] += real * grad_imag - imag * grad_real
                probe_real = probe_ref[0, here, lanes]
                probe_imag = probe_ref[1, here, lanes]
                turned[0].append(
                    pltpu.roll(probe_real * grad_real + probe_imag * grad_imag, col_at, 1)
                )
                turned[1].append(
                    pltpu.roll(probe_real * grad_imag - probe_imag * grad_real, col_at, 1)
                )
            for comp in range(2):
                first, second = turned[comp]
                canvas[comp, 0, there, :] += jnp.where(high, first, 0.0)
                canvas[comp, 1, there, :] += jnp.where(high, second, first)
                canvas[comp, 2, there, :] += jnp.where(high, 0.0, second)

    def group(g, carry):
        for u in range(together):
            make_psi(g * together + u, u)
            left_product(forward_ref, psi, half_wave, u)
        for u in range(together):
            right_product(half_wave, backward_ref, far, u)
        for u in range(together):
            make_chi(g * together + u, u)
            left_product(backward_ref, chi, back, u)
        for u in range(together):
            right_product(back, forward_ref, near, u)
        for u in range(together):
            scatter(g * together + u, u)
        return carry

    lax.fori_loop(0, count // together, group, 0)
    base = 2 * tall
    if cols == 2:
        tiles = (1, 2 * has_right.astype(jnp.int32))
        comps = ((col,), (1 - col,))
    else:
        tiles = (1, 0, 2)
        comps = ((0, 1), (), ())
    for out, tile, held in zip(outs, tiles, comps):
        for comp in range(2):
            out[pl.ds(comp * tall, tall), :] = canvas[comp, tile]
        for n, comp in enumerate(held):
            for j in range(2):
                out[pl.ds(base + (2 * n + j) * length, length), :] = probe_sum[comp, j]
        if held:
            out[pl.ds(base + 2 * len(held) * length, SUBS), :] = miss[...]


def split_kernel(beams, tall, length, *refs):
    spot_ref = refs[0]
    ins, outs = refs[1:-beams], refs[-beams:]
    part = tall // (2 * beams)
    strip = length // beams
    planes = (ins[0].shape[0] - 2 * tall - SUBS) // length

    def fetch(where):
        total = ins[0][where, :]
        for ref in ins[1:]:
            total = total + ref[where, :]
        return total

    for k in range(beams):
        quarter = jnp.bitwise_xor(spot_ref[0], k)
        spots = (quarter + beams // 2, lax.rem(quarter + 3 * beams // 2, 2 * beams))
        for which, at in enumerate(spots):
            for comp in range(2):
                where = pl.ds(pl.multiple_of(comp * tall + at * part, SUBS), part)
                outs[k][pl.ds((2 * which + comp) * part, part), :] = fetch(where)
        for n in range(planes):
            start = 2 * tall + n * length + quarter * strip
            where = pl.ds(pl.multiple_of(start, SUBS), strip)
            outs[k][pl.ds(4 * part + n * strip, strip), :] = fetch(where)
        where = pl.ds(2 * tall + planes * length, SUBS)
        outs[k][pl.ds(4 * part + planes * strip, SUBS), :] = fetch(where)


def final_kernel(beams, halves, planes, part, scale, total, *refs):
    spot_ref = refs[0]
    gathered = refs[1 : 1 + beams]
    if halves == 2:
        probes = [gathered, refs[1 + beams : 1 + 2 * beams]]
    else:
        probes = [gathered]
    object_ref, probe_ref, loss_ref, object_now, probe_now, sems = refs[-6:]
    strip = (gathered[0].shape[0] - 2 * SUBS - 2 * part) // planes
    length = strip * beams
    miss_at = pl.ds(planes * strip, SUBS)
    square_at = pl.ds(planes * strip + SUBS, SUBS)
    for k in range(beams):
        quarter = jnp.bitwise_xor(spot_ref[0], k)
        where = rows_of(quarter, strip)
        for h in range(halves):
            for n in range(planes):
                comp = (jnp.bitwise_xor(spot_ref[2], h)) if halves == 2 else n // 2
                lanes = pl.ds((n % 2) * LANES, LANES)
                probe_now[comp, where, lanes] = (
                    probes[h][k][pl.ds(n * strip, strip), :] * (1.0 / total)
                )
    copies = []
    for comp in range(2):
        for q in range(2):
            where = pl.ds(q * (length // 2), length // 2)
            copies.append((probe_now.at[comp, where], probe_ref.at[comp, where]))
    copies = [pltpu.make_async_copy(a, b, sems.at[i]) for i, (a, b) in enumerate(copies)]
    for copy in copies:
        copy.start()
    if halves == 2:
        squares = butterfly([ref[square_at, :] for ref in probes[0]])
        squares = squares + butterfly([ref[square_at, :] for ref in probes[1]])
    else:
        squares = refs[1 + beams][...]
    mean_square = jnp.sum(squares, keepdims=True) * scale
    factor = jnp.minimum(1.0, 0.5 / jnp.sqrt(mean_square + 1e-06))
    loss = jnp.sum(gathered[0][miss_at, :], keepdims=True) / (total * length * length)
    loss_ref[...] = jnp.broadcast_to(loss, loss_ref.shape)
    base = planes * strip + 2 * SUBS
    for k in range(beams):
        where = rows_of(jnp.bitwise_xor(spot_ref[0], k), part)
        for comp in range(2):
            object_now[comp, where, :] = gathered[k][pl.ds(base + comp * part, part), :] * factor
    for comp in range(2):
        copy = pltpu.make_async_copy(
            object_now.at[comp], object_ref.at[comp], sems.at[len(copies)]
        )
        copy.start()
        copies.append(copy)
    for copy in copies:
        copy.wait()


def call(kernel, shapes, scalars, arrays, scratch=(), flops=0, array_spec=VMEM, out_specs=None):
    size = sum(a.size * a.dtype.itemsize for a in arrays)
    return pl.pallas_call(
        kernel,
        out_shape=[jax.ShapeDtypeStruct(s, F32) for s in shapes],
        in_specs=[SMEM] * len(scalars) + [array_spec] * len(arrays),
        out_specs=out_specs or [VMEM] * len(shapes),
        scratch_shapes=list(scratch),
        compiler_params=pltpu.CompilerParams(vmem_limit_bytes=40 * 2**20),
        cost_estimate=pl.CostEstimate(flops=flops, bytes_accessed=size, transcendentals=0),
    )(*scalars, *arrays)


def wave_call(sizes, scalars, arrays):
    beams, cols, count, length, tall = sizes
    paired = cols == 2
    deep = 2 * tall + (2 if paired else 4) * length + SUBS
    shapes = [(deep, LANES)] * 2 if paired else [(deep, LANES)] + [(2 * tall, LANES)] * 2
    u = math.gcd(count, TOGETHER)
    return call(
        functools.partial(wave_kernel, beams, cols, count, length),
        shapes,
        scalars,
        arrays + [jnp.asarray(table) for table in dft_blocks(length)],
        [
            pltpu.VMEM((2, 3, tall, LANES), F32),
            pltpu.VMEM((2, 3, tall, LANES), F32),
            pltpu.VMEM((2, 2, length, LANES), F32),
            pltpu.VMEM((SUBS, LANES), F32),
            pltpu.VMEM((u, 2, 2, length, LANES), F32),
            pltpu.VMEM((u, 2 * length, length), BF16),
            pltpu.VMEM((u, length, 2 * length), BF16),
            pltpu.VMEM((u, length, 2 * length), F32),
            pltpu.VMEM((u, 2 * length, length), BF16),
            pltpu.VMEM((u, length, 2 * length), BF16),
            pltpu.VMEM((u, length, 2 * length), F32),
        ],
        flops=count * 32 * length**3,
    )


def local(phase_volume, absorb_volume, probe, amplitudes, scan_rows, scan_cols):
    length = probe.shape[1]
    count = scan_rows.shape[2]
    rows_local = phase_volume.shape[1]
    cols_local = phase_volume.shape[2]
    beams, rows, cols = (lax.axis_size(a) for a in ("beam", "row", "col"))
    assert cols_local == LANES and length == 2 * LANES and rows_local == length
    beam, row, col = (lax.axis_index(a) for a in ("beam", "row", "col"))
    spot = jnp.concatenate(
        [jnp.stack([beam, row, col]), scan_rows.reshape(count), scan_cols.reshape(count)]
    ).astype(jnp.int32)
    part = rows_local // beams
    tall = rows_local + length
    others = range(1, beams)
    near_half = beams // 2

    def toward(value, step):
        pairs = []
        for b in range(beams):
            way = step if b >= near_half else -step
            for r in range(rows):
                if 0 <= r + way < rows:
                    pairs.append((b * rows + r, b * rows + r + way))
        return lax.ppermute(value, ("beam", "row"), pairs)

    sums = call(
        functools.partial(sum_kernel, beams),
        [(2, part, LANES)] * beams,
        [spot],
        [phase_volume, absorb_volume],
        [
            pltpu.VMEM(phase_volume.shape, BF16),
            pltpu.VMEM(phase_volume.shape, BF16),
            pltpu.VMEM((beams, 2, part, LANES), F32),
            pltpu.SemaphoreType.DMA((2 * beams,)),
        ],
        array_spec=HBM,
    )
    got = [sums[0]] + [exchange(sums[k], "beam", k) for k in others]
    total = butterfly(got)
    total = jnp.stack([total, toward(total, 1)])
    damping = jnp.exp(-total[:, 1])
    own = jnp.stack([damping * jnp.cos(total[:, 0]), damping * jnp.sin(total[:, 0])], axis=1)
    trans = own[0]
    own = own.reshape(4, part, LANES)
    mids = [own] + [exchange(own, "beam", k) for k in others]
    if cols == 2:
        lefts = [exchange(x, "col", 1) for x in mids]
        rights = lefts
    else:
        lefts = [lax.ppermute(x, "col", [(i, i + 1) for i in range(cols - 1)]) for x in mids]
        rights = [lax.ppermute(x, "col", [(i + 1, i) for i in range(cols - 1)]) for x in mids]
    paired = cols == 2
    planes = 2 if paired else 4
    outs = wave_call(
        (beams, cols, count, length, tall),
        [spot],
        [*mids, *lefts, *rights, probe, amplitudes.reshape(count, length, length)],
    )
    if paired:
        pieces = [outs[0], exchange(outs[1], "col", 1)]
    else:
        keep, to_left, to_right = outs
        edge = lax.ppermute(to_left, "col", [(i + 1, i) for i in range(cols - 1)])
        edge = edge + lax.ppermute(to_right, "col", [(i, i + 1) for i in range(cols - 1)])
        rest = lax.psum(keep[2 * tall :], "col")
        pieces = [jnp.concatenate([keep[: 2 * tall] + edge, rest])]
    strip = length // beams
    flat = 4 * part + planes * strip + SUBS
    split = call(
        functools.partial(split_kernel, beams, tall, length),
        [(flat, LANES)] * beams,
        [spot],
        pieces,
    )

    got = [split[0]] + [exchange(split[k], "beam", k) for k in others]
    summed = butterfly(got)
    whole = summed[: 2 * part] + toward(summed[2 * part : 4 * part], -1)
    real, imag = whole[:part], whole[part:]
    grad_phase = trans[0] * imag - trans[1] * real
    grad_absorb = -(trans[0] * real + trans[1] * imag)
    squares = grad_phase * grad_phase + grad_absorb * grad_absorb
    squares = squares.reshape(part // SUBS, SUBS, LANES).sum(0)
    carried = jnp.concatenate([summed[4 * part :], squares])
    gradient = jnp.concatenate([grad_phase, grad_absorb])
    carried = butterfly(
        [carried] + [exchange(carried, "row", k) for k in range(1, rows)]
    )
    carried = jnp.concatenate([carried, gradient])
    gathered = [carried] + [exchange(carried, "beam", k) for k in others]
    at = planes * strip + SUBS
    if paired:
        more = [exchange(x[: at + SUBS], "col", 1) for x in gathered]
    else:
        more = [lax.psum(butterfly([x[at : at + SUBS] for x in gathered]), "col")]
    operands = gathered + more
    plane_devices = rows * cols
    objects_step, probe_gradient, loss = call(
        functools.partial(
            final_kernel,
            beams,
            2 if paired else 1,
            planes,
            part,
            1.0 / (2 * rows_local * cols_local * plane_devices),
            float(plane_devices * beams * count),
        ),
        [(2, rows_local, cols_local), (2, length, length), (1, 1)],
        [spot],
        operands,
        [
            pltpu.VMEM((2, rows_local, cols_local), F32),
            pltpu.VMEM((2, length, length), F32),
            pltpu.SemaphoreType.DMA((6,)),
        ],
        out_specs=[HBM, HBM, VMEM],
    )
    return objects_step, probe_gradient, loss[0, 0]


def solution(mesh):
    in_specs = (
        P("beam", "row", "col"),
        P("beam", "row", "col"),
        P(),
        P("row", "col", "beam", None, None),
        P("row", "col", "beam"),
        P("row", "col", "beam"),
    )
    out_specs = (P(None, "row", "col"), P(), P())
    return jax.shard_map(local, mesh=mesh, in_specs=in_specs, out_specs=out_specs, check_vma=False)
```

```python
import functools
import math

import jax
import jax.numpy as jnp
import numpy as np
from jax import lax
from jax.experimental import pallas as pl
from jax.experimental.pallas import tpu as pltpu
from jax.sharding import PartitionSpec as P

LANES = 128
SUBS = 8
CHUNK = 32
TOGETHER = 8
VMEM = pl.BlockSpec(memory_space=pltpu.VMEM)
SMEM = pl.BlockSpec(memory_space=pltpu.SMEM)
HBM = pl.BlockSpec(memory_space=pltpu.HBM)
F32 = jnp.float32
BF16 = jnp.bfloat16


def dft_blocks(length):
    indices = np.arange(length, dtype=np.int64)
    product = (indices[:, None] * indices[None, :] % length).astype(np.float32)
    angles = (product * np.float32(2.0 * math.pi / length)).astype(np.float64)
    factor = np.float32(1.0 / math.sqrt(length))
    real = (np.cos(angles).astype(np.float32) * factor).astype(jnp.bfloat16)
    imag = (-np.sin(angles).astype(np.float32) * factor).astype(jnp.bfloat16)
    forward = np.block([[real, -imag], [imag, real]])
    backward = np.block([[real, imag], [-imag, real]])
    return forward.astype(jnp.bfloat16), backward.astype(jnp.bfloat16)


def exchange(value, axis, mask):
    count = lax.axis_size(axis)
    return lax.ppermute(value, axis, [(i, i ^ mask) for i in range(count)])


def butterfly(values):
    while len(values) > 1:
        values = [values[i] + values[i + 1] for i in range(0, len(values), 2)]
    return values[0]


def rows_of(index, size):
    return pl.ds(pl.multiple_of(index * size, size), size)


def sum_kernel(beams, phase_ref, absorb_ref, *refs):
    outs, (phase_now, absorb_now, sums, sems) = refs[:beams], refs[beams:]
    part = phase_now.shape[1] // beams
    copies = []
    for q in range(beams):
        where = pl.ds(q * part, part)
        for comp, (a, b) in enumerate(((phase_ref, phase_now), (absorb_ref, absorb_now))):
            copy = pltpu.make_async_copy(
                a.at[:, where, :], b.at[:, where, :], sems.at[2 * q + comp]
            )
            copy.start()
            copies.append(copy)
    for q in range(beams):
        where = pl.ds(q * part, part)
        for comp, ref in enumerate((phase_now, absorb_now)):
            copies[2 * q + comp].wait()
            total = ref[0, where, :].astype(F32)
            for d in range(1, ref.shape[0]):
                total = total + ref[d, where, :].astype(F32)
            sums[q, comp] = total
    for k in range(beams):
        outs[k][...] = sums[jnp.bitwise_xor(lax.axis_index("beam"), k)]


def wave_kernel(beams, cols, count, length, *refs):
    spot_ref = refs[0]
    mid_refs = refs[1 : 1 + beams]
    left_refs = refs[1 + beams : 1 + 2 * beams]
    right_refs = refs[1 + 2 * beams : 1 + 3 * beams]
    probe_ref, amp_ref, forward_ref, backward_ref = refs[1 + 3 * beams : 5 + 3 * beams]
    sends = 1 if cols == 2 else 2
    outs = refs[5 + 3 * beams : 6 + 3 * beams + sends]
    cells, canvas, probe_sum, miss, trans, psi, half_wave, far, chi, back, near = refs[
        6 + 3 * beams + sends :
    ]
    part = mid_refs[0].shape[1]
    tall = cells.shape[2]
    together = trans.shape[0]
    beam, col = lax.axis_index("beam"), lax.axis_index("col")
    has_left, has_right = col > 0, col < cols - 1
    for k in range(beams):
        quarter = jnp.bitwise_xor(beam, k)
        spots = (quarter + beams // 2, lax.rem(quarter + 3 * beams // 2, 2 * beams))
        for which, at in enumerate(spots):
            where = rows_of(at, part)
            for comp in range(2):
                outside = 1.0 - comp
                source = 2 * which + comp
                cells[comp, 0, where, :] = jnp.where(has_left, left_refs[k][source], outside)
                cells[comp, 1, where, :] = mid_refs[k][source]
                cells[comp, 2, where, :] = jnp.where(has_right, right_refs[k][source], outside)
    canvas[...] = jnp.zeros_like(canvas)
    probe_sum[...] = jnp.zeros_like(probe_sum)
    miss[...] = jnp.zeros_like(miss)
    lane = lax.broadcasted_iota(jnp.int32, (CHUNK, LANES), 1)
    chunks = length // CHUNK

    def make_psi(s, u):
        row_at, col_at = spot_ref[s], spot_ref[count + s]
        back_shift = lax.rem(LANES - col_at, LANES)
        low = lane < LANES - col_at
        for i in range(chunks):
            here = pl.ds(i * CHUNK, CHUNK)
            there = pl.ds(row_at + i * CHUNK, CHUNK)
            pieces = []
            for comp in range(2):
                turned = [
                    pltpu.roll(cells[comp, j, there, :], back_shift, 1) for j in range(3)
                ]
                pieces.append([jnp.where(low, turned[j], turned[j + 1]) for j in range(2)])
            for j in range(2):
                lanes = pl.ds(j * LANES, LANES)
                real, imag = pieces[0][j], pieces[1][j]
                trans[u, 0, j, here, :] = real
                trans[u, 1, j, here, :] = imag
                probe_real = probe_ref[0, here, lanes]
                probe_imag = probe_ref[1, here, lanes]
                psi[u, here, lanes] = (probe_real * real - probe_imag * imag).astype(BF16)
                psi[u, pl.ds(length + i * CHUNK, CHUNK), lanes] = (
                    probe_real * imag + probe_imag * real
                ).astype(BF16)

    def left_product(table, source, target, u):
        result = jnp.dot(table[...], source[u], preferred_element_type=F32).astype(BF16)
        target[u, :, :length] = result[:length]
        target[u, :, length:] = result[length:]

    def right_product(source, table, target, u):
        target[u] = jnp.dot(source[u], table[...], preferred_element_type=F32)

    def make_chi(s, u):
        for i in range(chunks):
            here = pl.ds(i * CHUNK, CHUNK)
            real, imag = far[u, here, :length], far[u, here, length:]
            amplitude = amp_ref[s, here, :].astype(F32)
            power = real * real + imag * imag
            off = jnp.sqrt(power) - amplitude
            wide = off * off
            wide = wide[:, :LANES] + wide[:, LANES:]
            miss[...] += wide.reshape(CHUNK // SUBS, SUBS, LANES).sum(0)
            ratio = 1.0 - amplitude * lax.rsqrt(jnp.maximum(power, 0.25))
            chi[u, here, :] = (real * ratio).astype(BF16)
            chi[u, pl.ds(length + i * CHUNK, CHUNK), :] = (imag * ratio).astype(BF16)

    def scatter(s, u):
        row_at, col_at = spot_ref[s], spot_ref[count + s]
        high = lane >= col_at
        for i in range(chunks):
            here = pl.ds(i * CHUNK, CHUNK)
            there = pl.ds(row_at + i * CHUNK, CHUNK)
            turned = [[], []]
            for j in range(2):
                lanes = pl.ds(j * LANES, LANES)
                grad_real = near[u, here, lanes]
                grad_imag = near[u, here, pl.ds(length + j * LANES, LANES)]
                real, imag = trans[u, 0, j, here, :], trans[u, 1, j, here, :]
                probe_sum[0, j, here, :] += real * grad_real + imag * grad_imag
                probe_sum[1, j, here, :] += real * grad_imag - imag * grad_real
                probe_real = probe_ref[0, here, lanes]
                probe_imag = probe_ref[1, here, lanes]
                turned[0].append(
                    pltpu.roll(probe_real * grad_real + probe_imag * grad_imag, col_at, 1)
                )
                turned[1].append(
                    pltpu.roll(probe_real * grad_imag - probe_imag * grad_real, col_at, 1)
                )
            for comp in range(2):
                first, second = turned[comp]
                canvas[comp, 0, there, :] += jnp.where(high, first, 0.0)
                canvas[comp, 1, there, :] += jnp.where(high, second, first)
                canvas[comp, 2, there, :] += jnp.where(high, 0.0, second)

    def group(g, carry):
        for u in range(together):
            make_psi(g * together + u, u)
            left_product(forward_ref, psi, half_wave, u)
        for u in range(together):
            right_product(half_wave, backward_ref, far, u)
        for u in range(together):
            make_chi(g * together + u, u)
            left_product(backward_ref, chi, back, u)
        for u in range(together):
            right_product(back, forward_ref, near, u)
        for u in range(together):
            scatter(g * together + u, u)
        return carry

    lax.fori_loop(0, count // together, group, 0)
    base = 2 * tall
    if cols == 2:
        tiles = (1, 2 * has_right.astype(jnp.int32))
        comps = ((col,), (1 - col,))
    else:
        tiles = (1, 0, 2)
        comps = ((0, 1), (), ())
    for out, tile, held in zip(outs, tiles, comps):
        for comp in range(2):
            out[pl.ds(comp * tall, tall), :] = canvas[comp, tile]
        for n, comp in enumerate(held):
            for j in range(2):
                out[pl.ds(base + (2 * n + j) * length, length), :] = probe_sum[comp, j]
        if held:
            out[pl.ds(base + 2 * len(held) * length, SUBS), :] = miss[...]


def split_kernel(beams, tall, length, *refs):
    beam = lax.axis_index("beam")
    ins, outs = refs[:-beams], refs[-beams:]
    part = tall // (2 * beams)
    strip = length // beams
    planes = (ins[0].shape[0] - 2 * tall - SUBS) // length

    def fetch(where):
        total = ins[0][where, :]
        for ref in ins[1:]:
            total = total + ref[where, :]
        return total

    for k in range(beams):
        quarter = jnp.bitwise_xor(beam, k)
        spots = (quarter + beams // 2, lax.rem(quarter + 3 * beams // 2, 2 * beams))
        for which, at in enumerate(spots):
            for comp in range(2):
                where = pl.ds(pl.multiple_of(comp * tall + at * part, SUBS), part)
                outs[k][pl.ds((2 * which + comp) * part, part), :] = fetch(where)
        for n in range(planes):
            start = 2 * tall + n * length + quarter * strip
            where = pl.ds(pl.multiple_of(start, SUBS), strip)
            outs[k][pl.ds(4 * part + n * strip, strip), :] = fetch(where)
        where = pl.ds(2 * tall + planes * length, SUBS)
        outs[k][pl.ds(4 * part + planes * strip, SUBS), :] = fetch(where)


def final_kernel(beams, halves, planes, part, scale, total, *refs):
    beam, col = lax.axis_index("beam"), lax.axis_index("col")
    gathered = refs[:beams]
    if halves == 2:
        probes = [gathered, refs[beams : 2 * beams]]
    else:
        probes = [gathered]
    object_ref, probe_ref, loss_ref = refs[-3:]
    strip = (gathered[0].shape[0] - 2 * SUBS - 2 * part) // planes
    length = strip * beams
    miss_at = pl.ds(planes * strip, SUBS)
    square_at = pl.ds(planes * strip + SUBS, SUBS)
    for k in range(beams):
        quarter = jnp.bitwise_xor(beam, k)
        where = rows_of(quarter, strip)
        for h in range(halves):
            for n in range(planes):
                comp = (jnp.bitwise_xor(col, h)) if halves == 2 else n // 2
                lanes = pl.ds((n % 2) * LANES, LANES)
                probe_ref[comp, where, lanes] = (
                    probes[h][k][pl.ds(n * strip, strip), :] * (1.0 / total)
                )
    if halves == 2:
        squares = butterfly([ref[square_at, :] for ref in probes[0]])
        squares = squares + butterfly([ref[square_at, :] for ref in probes[1]])
    else:
        squares = refs[beams][...]
    mean_square = jnp.sum(squares, keepdims=True) * scale
    factor = jnp.minimum(1.0, 0.5 / jnp.sqrt(mean_square + 1e-06))
    loss = jnp.sum(gathered[0][miss_at, :], keepdims=True) / (total * length * length)
    loss_ref[...] = jnp.broadcast_to(loss, loss_ref.shape)
    base = planes * strip + 2 * SUBS
    for k in range(beams):
        where = rows_of(jnp.bitwise_xor(beam, k), part)
        for comp in range(2):
            object_ref[comp, where, :] = gathered[k][pl.ds(base + comp * part, part), :] * factor


def call(kernel, shapes, scalars, arrays, scratch=(), flops=0, array_spec=VMEM, limit=40 * 2**20):
    size = sum(a.size * a.dtype.itemsize for a in arrays)
    return pl.pallas_call(
        kernel,
        out_shape=[jax.ShapeDtypeStruct(s, F32) for s in shapes],
        in_specs=[SMEM] * len(scalars) + [array_spec] * len(arrays),
        out_specs=[VMEM] * len(shapes),
        scratch_shapes=list(scratch),
        compiler_params=pltpu.CompilerParams(vmem_limit_bytes=limit),
        cost_estimate=pl.CostEstimate(flops=flops, bytes_accessed=size, transcendentals=0),
    )(*scalars, *arrays)


def wave_call(sizes, scalars, arrays):
    beams, cols, count, length, tall = sizes
    paired = cols == 2
    deep = 2 * tall + (2 if paired else 4) * length + SUBS
    shapes = [(deep, LANES)] * 2 if paired else [(deep, LANES)] + [(2 * tall, LANES)] * 2
    u = math.gcd(count, TOGETHER)
    return call(
        functools.partial(wave_kernel, beams, cols, count, length),
        shapes,
        scalars,
        arrays + [jnp.asarray(table) for table in dft_blocks(length)],
        [
            pltpu.VMEM((2, 3, tall, LANES), F32),
            pltpu.VMEM((2, 3, tall, LANES), F32),
            pltpu.VMEM((2, 2, length, LANES), F32),
            pltpu.VMEM((SUBS, LANES), F32),
            pltpu.VMEM((u, 2, 2, length, LANES), F32),
            pltpu.VMEM((u, 2 * length, length), BF16),
            pltpu.VMEM((u, length, 2 * length), BF16),
            pltpu.VMEM((u, length, 2 * length), F32),
            pltpu.VMEM((u, 2 * length, length), BF16),
            pltpu.VMEM((u, length, 2 * length), BF16),
            pltpu.VMEM((u, length, 2 * length), F32),
        ],
        flops=count * 32 * length**3,
    )


def local(phase_volume, absorb_volume, probe, amplitudes, scan_rows, scan_cols):
    length = probe.shape[1]
    count = scan_rows.shape[2]
    rows_local = phase_volume.shape[1]
    cols_local = phase_volume.shape[2]
    beams, rows, cols = (lax.axis_size(a) for a in ("beam", "row", "col"))
    assert cols_local == LANES and length == 2 * LANES and rows_local == length
    places = jnp.concatenate([scan_rows.reshape(count), scan_cols.reshape(count)])
    part = rows_local // beams
    tall = rows_local + length
    others = range(1, beams)
    near_half = beams // 2

    def toward(value, step):
        pairs = []
        for b in range(beams):
            way = step if b >= near_half else -step
            for r in range(rows):
                if 0 <= r + way < rows:
                    pairs.append((b * rows + r, b * rows + r + way))
        return lax.ppermute(value, ("beam", "row"), pairs)

    sums = call(
        functools.partial(sum_kernel, beams),
        [(2, part, LANES)] * beams,
        [],
        [pltpu.with_memory_space_constraint(x, pltpu.HBM) for x in (phase_volume, absorb_volume)],
        [
            pltpu.VMEM(phase_volume.shape, BF16),
            pltpu.VMEM(phase_volume.shape, BF16),
            pltpu.VMEM((beams, 2, part, LANES), F32),
            pltpu.SemaphoreType.DMA((2 * beams,)),
        ],
        array_spec=HBM,
    )
    got = [sums[0]] + [exchange(sums[k], "beam", k) for k in others]
    total, places = lax.optimization_barrier((butterfly(got), places))
    total = jnp.stack([total, toward(total, 1)])
    damping = jnp.exp(-total[:, 1])
    own = jnp.stack([damping * jnp.cos(total[:, 0]), damping * jnp.sin(total[:, 0])], axis=1)
    trans = own[0]
    own = own.reshape(4, part, LANES)
    mids = [own] + [exchange(own, "beam", k) for k in others]
    if cols == 2:
        lefts = [exchange(x, "col", 1) for x in mids]
        rights = lefts
    else:
        lefts = [lax.ppermute(x, "col", [(i, i + 1) for i in range(cols - 1)]) for x in mids]
        rights = [lax.ppermute(x, "col", [(i + 1, i) for i in range(cols - 1)]) for x in mids]
    paired = cols == 2
    planes = 2 if paired else 4
    outs = wave_call(
        (beams, cols, count, length, tall),
        [places],
        [*mids, *lefts, *rights, probe, amplitudes.reshape(count, length, length)],
    )
    if paired:
        pieces = [outs[0], exchange(outs[1], "col", 1)]
    else:
        keep, to_left, to_right = outs
        edge = lax.ppermute(to_left, "col", [(i + 1, i) for i in range(cols - 1)])
        edge = edge + lax.ppermute(to_right, "col", [(i, i + 1) for i in range(cols - 1)])
        rest = lax.psum(keep[2 * tall :], "col")
        pieces = [jnp.concatenate([keep[: 2 * tall] + edge, rest])]
    strip = length // beams
    flat = 4 * part + planes * strip + SUBS
    split = call(
        functools.partial(split_kernel, beams, tall, length),
        [(flat, LANES)] * beams,
        [],
        pieces,
    )

    got = [split[0]] + [exchange(split[k], "beam", k) for k in others]
    summed = butterfly(got)
    whole = summed[: 2 * part] + toward(summed[2 * part : 4 * part], -1)
    real, imag = whole[:part], whole[part:]
    grad_phase = trans[0] * imag - trans[1] * real
    grad_absorb = -(trans[0] * real + trans[1] * imag)
    squares = grad_phase * grad_phase + grad_absorb * grad_absorb
    squares = squares.reshape(part // SUBS, SUBS, LANES).sum(0)
    carried = jnp.concatenate([summed[4 * part :], squares])
    gradient = jnp.concatenate([grad_phase, grad_absorb])
    carried = butterfly(
        [carried] + [exchange(carried, "row", k) for k in range(1, rows)]
    )
    carried = jnp.concatenate([carried, gradient])
    gathered = [carried] + [exchange(carried, "beam", k) for k in others]
    at = planes * strip + SUBS
    if paired:
        more = [exchange(x[: at + SUBS], "col", 1) for x in gathered]
    else:
        more = [lax.psum(butterfly([x[at : at + SUBS] for x in gathered]), "col")]
    operands = gathered + more
    plane_devices = rows * cols
    objects_step, probe_gradient, loss = call(
        functools.partial(
            final_kernel,
            beams,
            2 if paired else 1,
            planes,
            part,
            1.0 / (2 * rows_local * cols_local * plane_devices),
            float(plane_devices * beams * count),
        ),
        [(2, rows_local, cols_local), (2, length, length), (1, 1)],
        [],
        operands,
    )
    return objects_step, probe_gradient, loss[0, 0]


def solution(mesh):
    in_specs = (
        P("beam", "row", "col"),
        P("beam", "row", "col"),
        P(),
        P("row", "col", "beam", None, None),
        P("row", "col", "beam"),
        P("row", "col", "beam"),
    )
    out_specs = (P(None, "row", "col"), P(), P())
    return jax.shard_map(local, mesh=mesh, in_specs=in_specs, out_specs=out_specs, check_vma=False)
```

```python
import functools
import math

import jax
import jax.numpy as jnp
import numpy as np
from jax import lax
from jax.experimental import pallas as pl
from jax.experimental.pallas import tpu as pltpu
from jax.sharding import PartitionSpec as P

LANES = 128
SUBS = 8
CHUNK = 32
TOGETHER = 8
VMEM = pl.BlockSpec(memory_space=pltpu.VMEM)
SMEM = pl.BlockSpec(memory_space=pltpu.SMEM)
HBM = pl.BlockSpec(memory_space=pltpu.HBM)
F32 = jnp.float32
BF16 = jnp.bfloat16


def dft_blocks(length):
    indices = np.arange(length, dtype=np.int64)
    product = (indices[:, None] * indices[None, :] % length).astype(np.float32)
    angles = (product * np.float32(2.0 * math.pi / length)).astype(np.float64)
    factor = np.float32(1.0 / math.sqrt(length))
    real = (np.cos(angles).astype(np.float32) * factor).astype(jnp.bfloat16)
    imag = (-np.sin(angles).astype(np.float32) * factor).astype(jnp.bfloat16)
    forward = np.block([[real, -imag], [imag, real]])
    backward = np.block([[real, imag], [-imag, real]])
    return forward.astype(jnp.bfloat16), backward.astype(jnp.bfloat16)


def exchange(value, axis, mask):
    count = lax.axis_size(axis)
    return lax.ppermute(value, axis, [(i, i ^ mask) for i in range(count)])


def butterfly(values):
    while len(values) > 1:
        values = [values[i] + values[i + 1] for i in range(0, len(values), 2)]
    return values[0]


def rows_of(index, size):
    return pl.ds(pl.multiple_of(index * size, size), size)


def sum_kernel(beams, phase_ref, absorb_ref, *refs):
    outs, (phase_now, absorb_now, sums, sems) = refs[:beams], refs[beams:]
    part = phase_now.shape[1] // beams
    copies = []
    for q in range(beams):
        where = pl.ds(q * part, part)
        for comp, (a, b) in enumerate(((phase_ref, phase_now), (absorb_ref, absorb_now))):
            copy = pltpu.make_async_copy(
                a.at[:, where, :], b.at[:, where, :], sems.at[2 * q + comp]
            )
            copy.start()
            copies.append(copy)
    for q in range(beams):
        where = pl.ds(q * part, part)
        for comp, ref in enumerate((phase_now, absorb_now)):
            copies[2 * q + comp].wait()
            total = ref[0, where, :].astype(F32)
            for d in range(1, ref.shape[0]):
                total = total + ref[d, where, :].astype(F32)
            sums[q, comp] = total
    for k in range(beams):
        outs[k][...] = sums[jnp.bitwise_xor(lax.axis_index("beam"), k)]


def wave_kernel(beams, cols, count, length, *refs):
    spot_ref = refs[0]
    held = 2 * beams
    mid_refs, left_refs, right_refs = (refs[1 + i * held : 1 + (i + 1) * held] for i in range(3))
    refs = refs[1 + 3 * held :]
    probe_ref, amp_ref, forward_ref, backward_ref = refs[:4]
    sends = 1 if cols == 2 else 2
    outs = refs[4 : 5 + sends]
    cells, canvas, probe_sum, miss, trans, psi, half_wave, far, chi, back, near = refs[
        5 + sends : -2
    ]
    scan_ref, scan_sem = refs[-2:]
    fetch = pltpu.make_async_copy(spot_ref, scan_ref, scan_sem)
    fetch.start()
    part = mid_refs[0].shape[1]
    tall = cells.shape[2]
    together = trans.shape[0]
    beam, col = lax.axis_index("beam"), lax.axis_index("col")
    has_left, has_right = col > 0, col < cols - 1
    for k in range(beams):
        quarter = jnp.bitwise_xor(beam, k)
        spots = (quarter + beams // 2, lax.rem(quarter + 3 * beams // 2, 2 * beams))
        for which, at in enumerate(spots):
            where = rows_of(at, part)
            for comp in range(2):
                outside = 1.0 - comp
                source = which * beams + k
                cells[comp, 0, where, :] = jnp.where(has_left, left_refs[source][comp], outside)
                cells[comp, 1, where, :] = mid_refs[source][comp]
                cells[comp, 2, where, :] = jnp.where(has_right, right_refs[source][comp], outside)
    canvas[...] = jnp.zeros_like(canvas)
    probe_sum[...] = jnp.zeros_like(probe_sum)
    miss[...] = jnp.zeros_like(miss)
    lane = lax.broadcasted_iota(jnp.int32, (CHUNK, LANES), 1)
    chunks = length // CHUNK
    fetch.wait()

    def make_psi(s, u):
        row_at, col_at = scan_ref[s], scan_ref[count + s]
        back_shift = lax.rem(LANES - col_at, LANES)
        low = lane < LANES - col_at
        for i in range(chunks):
            here = pl.ds(i * CHUNK, CHUNK)
            there = pl.ds(row_at + i * CHUNK, CHUNK)
            pieces = []
            for comp in range(2):
                turned = [
                    pltpu.roll(cells[comp, j, there, :], back_shift, 1) for j in range(3)
                ]
                pieces.append([jnp.where(low, turned[j], turned[j + 1]) for j in range(2)])
            for j in range(2):
                lanes = pl.ds(j * LANES, LANES)
                real, imag = pieces[0][j], pieces[1][j]
                trans[u, 0, j, here, :] = real
                trans[u, 1, j, here, :] = imag
                probe_real = probe_ref[0, here, lanes]
                probe_imag = probe_ref[1, here, lanes]
                psi[u, here, lanes] = (probe_real * real - probe_imag * imag).astype(BF16)
                psi[u, pl.ds(length + i * CHUNK, CHUNK), lanes] = (
                    probe_real * imag + probe_imag * real
                ).astype(BF16)

    def left_product(table, source, target, u):
        result = jnp.dot(table[...], source[u], preferred_element_type=F32).astype(BF16)
        target[u, :, :length] = result[:length]
        target[u, :, length:] = result[length:]

    def right_product(source, table, target, u):
        target[u] = jnp.dot(source[u], table[...], preferred_element_type=F32)

    def make_chi(s, u):
        for i in range(chunks):
            here = pl.ds(i * CHUNK, CHUNK)
            real, imag = far[u, here, :length], far[u, here, length:]
            amplitude = amp_ref[s, here, :].astype(F32)
            power = real * real + imag * imag
            off = jnp.sqrt(power) - amplitude
            wide = off * off
            wide = wide[:, :LANES] + wide[:, LANES:]
            miss[...] += wide.reshape(CHUNK // SUBS, SUBS, LANES).sum(0)
            ratio = 1.0 - amplitude * lax.rsqrt(jnp.maximum(power, 0.25))
            chi[u, here, :] = (real * ratio).astype(BF16)
            chi[u, pl.ds(length + i * CHUNK, CHUNK), :] = (imag * ratio).astype(BF16)

    def scatter(s, u):
        row_at, col_at = scan_ref[s], scan_ref[count + s]
        high = lane >= col_at
        for i in range(chunks):
            here = pl.ds(i * CHUNK, CHUNK)
            there = pl.ds(row_at + i * CHUNK, CHUNK)
            turned = [[], []]
            for j in range(2):
                lanes = pl.ds(j * LANES, LANES)
                grad_real = near[u, here, lanes]
                grad_imag = near[u, here, pl.ds(length + j * LANES, LANES)]
                real, imag = trans[u, 0, j, here, :], trans[u, 1, j, here, :]
                probe_sum[0, j, here, :] += real * grad_real + imag * grad_imag
                probe_sum[1, j, here, :] += real * grad_imag - imag * grad_real
                probe_real = probe_ref[0, here, lanes]
                probe_imag = probe_ref[1, here, lanes]
                turned[0].append(
                    pltpu.roll(probe_real * grad_real + probe_imag * grad_imag, col_at, 1)
                )
                turned[1].append(
                    pltpu.roll(probe_real * grad_imag - probe_imag * grad_real, col_at, 1)
                )
            for comp in range(2):
                first, second = turned[comp]
                canvas[comp, 0, there, :] += jnp.where(high, first, 0.0)
                canvas[comp, 1, there, :] += jnp.where(high, second, first)
                canvas[comp, 2, there, :] += jnp.where(high, 0.0, second)

    def group(g, carry):
        for u in range(together):
            make_psi(g * together + u, u)
            left_product(forward_ref, psi, half_wave, u)
        for u in range(together):
            right_product(half_wave, backward_ref, far, u)
        for u in range(together):
            make_chi(g * together + u, u)
            left_product(backward_ref, chi, back, u)
        for u in range(together):
            right_product(back, forward_ref, near, u)
        for u in range(together):
            scatter(g * together + u, u)
        return carry

    lax.fori_loop(0, count // together, group, 0)
    base = 2 * tall
    if cols == 2:
        tiles = (1, 2 * has_right.astype(jnp.int32))
        comps = ((col,), (1 - col,))
    else:
        tiles = (1, 0, 2)
        comps = ((0, 1), (), ())
    for out, tile, held in zip(outs, tiles, comps):
        for comp in range(2):
            out[pl.ds(comp * tall, tall), :] = canvas[comp, tile]
        for n, comp in enumerate(held):
            for j in range(2):
                out[pl.ds(base + (2 * n + j) * length, length), :] = probe_sum[comp, j]
        if held:
            out[pl.ds(base + 2 * len(held) * length, SUBS), :] = miss[...]


def split_kernel(beams, tall, length, *refs):
    beam = lax.axis_index("beam")
    ins, outs, edges = refs[: -2 * beams], refs[-2 * beams : -beams], refs[-beams:]
    part = tall // (2 * beams)
    strip = length // beams
    planes = (ins[0].shape[0] - 2 * tall - SUBS) // length

    def fetch(where):
        total = ins[0][where, :]
        for ref in ins[1:]:
            total = total + ref[where, :]
        return total

    for k in range(beams):
        quarter = jnp.bitwise_xor(beam, k)
        spots = (quarter + beams // 2, lax.rem(quarter + 3 * beams // 2, 2 * beams))
        for out, at in zip((outs[k], edges[k]), spots):
            for comp in range(2):
                where = pl.ds(pl.multiple_of(comp * tall + at * part, SUBS), part)
                out[pl.ds(comp * part, part), :] = fetch(where)
        for n in range(planes):
            start = 2 * tall + n * length + quarter * strip
            where = pl.ds(pl.multiple_of(start, SUBS), strip)
            outs[k][pl.ds(2 * part + n * strip, strip), :] = fetch(where)
        where = pl.ds(2 * tall + planes * length, SUBS)
        outs[k][pl.ds(2 * part + planes * strip, SUBS), :] = fetch(where)


def final_kernel(beams, halves, planes, part, scale, total, *refs):
    beam, col = lax.axis_index("beam"), lax.axis_index("col")
    gathered = refs[:beams]
    if halves == 2:
        probes = [gathered, refs[beams : 2 * beams]]
    else:
        probes = [gathered]
    object_ref, probe_ref, loss_ref = refs[-3:]
    strip = (gathered[0].shape[0] - 2 * SUBS - 2 * part) // planes
    length = strip * beams
    miss_at = pl.ds(planes * strip, SUBS)
    square_at = pl.ds(planes * strip + SUBS, SUBS)
    for k in range(beams):
        quarter = jnp.bitwise_xor(beam, k)
        where = rows_of(quarter, strip)
        for h in range(halves):
            for n in range(planes):
                comp = (jnp.bitwise_xor(col, h)) if halves == 2 else n // 2
                lanes = pl.ds((n % 2) * LANES, LANES)
                probe_ref[comp, where, lanes] = (
                    probes[h][k][pl.ds(n * strip, strip), :] * (1.0 / total)
                )
    if halves == 2:
        squares = butterfly([ref[square_at, :] for ref in probes[0]])
        squares = squares + butterfly([ref[square_at, :] for ref in probes[1]])
    else:
        squares = refs[beams][...]
    mean_square = jnp.sum(squares, keepdims=True) * scale
    factor = jnp.minimum(1.0, 0.5 / jnp.sqrt(mean_square + 1e-06))
    loss = jnp.sum(gathered[0][miss_at, :], keepdims=True) / (total * length * length)
    loss_ref[...] = jnp.broadcast_to(loss, loss_ref.shape)
    base = planes * strip + 2 * SUBS
    for k in range(beams):
        where = rows_of(jnp.bitwise_xor(beam, k), part)
        for comp in range(2):
            object_ref[comp, where, :] = gathered[k][pl.ds(base + comp * part, part), :] * factor


def call(kernel, shapes, scalars, arrays, scratch=(), flops=0, array_spec=VMEM, limit=40 * 2**20):
    size = sum(a.size * a.dtype.itemsize for a in arrays)
    return pl.pallas_call(
        kernel,
        out_shape=[jax.ShapeDtypeStruct(s, F32) for s in shapes],
        in_specs=[SMEM] * len(scalars) + [array_spec] * len(arrays),
        out_specs=[VMEM] * len(shapes),
        scratch_shapes=list(scratch),
        compiler_params=pltpu.CompilerParams(vmem_limit_bytes=limit),
        cost_estimate=pl.CostEstimate(flops=flops, bytes_accessed=size, transcendentals=0),
    )(*scalars, *arrays)


def wave_call(sizes, scalars, arrays):
    beams, cols, count, length, tall = sizes
    paired = cols == 2
    deep = 2 * tall + (2 if paired else 4) * length + SUBS
    shapes = [(deep, LANES)] * 2 if paired else [(deep, LANES)] + [(2 * tall, LANES)] * 2
    u = math.gcd(count, TOGETHER)
    return call(
        functools.partial(wave_kernel, beams, cols, count, length),
        shapes,
        scalars,
        arrays + [jnp.asarray(table) for table in dft_blocks(length)],
        [
            pltpu.VMEM((2, 3, tall, LANES), F32),
            pltpu.VMEM((2, 3, tall, LANES), F32),
            pltpu.VMEM((2, 2, length, LANES), F32),
            pltpu.VMEM((SUBS, LANES), F32),
            pltpu.VMEM((u, 2, 2, length, LANES), F32),
            pltpu.VMEM((u, 2 * length, length), BF16),
            pltpu.VMEM((u, length, 2 * length), BF16),
            pltpu.VMEM((u, length, 2 * length), F32),
            pltpu.VMEM((u, 2 * length, length), BF16),
            pltpu.VMEM((u, length, 2 * length), BF16),
            pltpu.VMEM((u, length, 2 * length), F32),
            pltpu.SMEM((2 * count,), jnp.int32),
            pltpu.SemaphoreType.DMA,
        ],
        flops=count * 32 * length**3,
    )


def local(phase_volume, absorb_volume, probe, amplitudes, scan_rows, scan_cols):
    length = probe.shape[1]
    count = scan_rows.shape[2]
    rows_local = phase_volume.shape[1]
    cols_local = phase_volume.shape[2]
    beams, rows, cols = (lax.axis_size(a) for a in ("beam", "row", "col"))
    assert cols_local == LANES and length == 2 * LANES and rows_local == length
    places = jnp.concatenate([scan_rows.reshape(count), scan_cols.reshape(count)])
    part = rows_local // beams
    tall = rows_local + length
    others = range(1, beams)
    near_half = beams // 2

    def toward(value, step):
        pairs = []
        for b in range(beams):
            way = step if b >= near_half else -step
            for r in range(rows):
                if 0 <= r + way < rows:
                    pairs.append((b * rows + r, b * rows + r + way))
        return lax.ppermute(value, ("beam", "row"), pairs)

    sums = call(
        functools.partial(sum_kernel, beams),
        [(2, part, LANES)] * beams,
        [],
        [pltpu.with_memory_space_constraint(x, pltpu.HBM) for x in (phase_volume, absorb_volume)],
        [
            pltpu.VMEM(phase_volume.shape, BF16),
            pltpu.VMEM(phase_volume.shape, BF16),
            pltpu.VMEM((beams, 2, part, LANES), F32),
            pltpu.SemaphoreType.DMA((2 * beams,)),
        ],
        array_spec=HBM,
    )
    got = [sums[0]] + [exchange(sums[k], "beam", k) for k in others]
    total, places = lax.optimization_barrier((butterfly(got), places))
    near = toward(total, 1)

    def spread(values):
        damping = jnp.exp(-values[1])
        wave = jnp.stack([damping * jnp.cos(values[0]), damping * jnp.sin(values[0])])
        return wave, [wave] + [exchange(wave, "beam", k) for k in others]

    trans, mids = spread(total)
    mids = mids + spread(near)[1]
    if cols == 2:
        lefts = [exchange(x, "col", 1) for x in mids]
        rights = lefts
    else:
        lefts = [lax.ppermute(x, "col", [(i, i + 1) for i in range(cols - 1)]) for x in mids]
        rights = [lax.ppermute(x, "col", [(i + 1, i) for i in range(cols - 1)]) for x in mids]
    paired = cols == 2
    planes = 2 if paired else 4
    outs = wave_call(
        (beams, cols, count, length, tall),
        [],
        [places, *mids, *lefts, *rights, probe, amplitudes.reshape(count, length, length)],
    )
    if paired:
        pieces = [outs[0], exchange(outs[1], "col", 1)]
    else:
        keep, to_left, to_right = outs
        edge = lax.ppermute(to_left, "col", [(i + 1, i) for i in range(cols - 1)])
        edge = edge + lax.ppermute(to_right, "col", [(i, i + 1) for i in range(cols - 1)])
        rest = lax.psum(keep[2 * tall :], "col")
        pieces = [jnp.concatenate([keep[: 2 * tall] + edge, rest])]
    strip = length // beams
    flat = 2 * part + planes * strip + SUBS
    split = call(
        functools.partial(split_kernel, beams, tall, length),
        [(flat, LANES)] * beams + [(2 * part, LANES)] * beams,
        [],
        pieces,
    )

    edges = [split[beams]] + [exchange(split[beams + k], "beam", k) for k in others]
    edge = toward(butterfly(edges), -1)
    summed = butterfly([split[0]] + [exchange(split[k], "beam", k) for k in others])
    whole = summed[: 2 * part] + edge
    real, imag = whole[:part], whole[part:]
    grad_phase = trans[0] * imag - trans[1] * real
    grad_absorb = -(trans[0] * real + trans[1] * imag)
    squares = grad_phase * grad_phase + grad_absorb * grad_absorb
    squares = squares.reshape(part // SUBS, SUBS, LANES).sum(0)
    carried = jnp.concatenate([summed[2 * part :], squares])
    gradient = jnp.concatenate([grad_phase, grad_absorb])
    carried = butterfly(
        [carried] + [exchange(carried, "row", k) for k in range(1, rows)]
    )
    carried = jnp.concatenate([carried, gradient])
    gathered = [carried] + [exchange(carried, "beam", k) for k in others]
    at = planes * strip + SUBS
    if paired:
        more = [exchange(x[: at + SUBS], "col", 1) for x in gathered]
    else:
        more = [lax.psum(butterfly([x[at : at + SUBS] for x in gathered]), "col")]
    operands = gathered + more
    plane_devices = rows * cols
    objects_step, probe_gradient, loss = call(
        functools.partial(
            final_kernel,
            beams,
            2 if paired else 1,
            planes,
            part,
            1.0 / (2 * rows_local * cols_local * plane_devices),
            float(plane_devices * beams * count),
        ),
        [(2, rows_local, cols_local), (2, length, length), (1, 1)],
        [],
        operands,
    )
    return objects_step, probe_gradient, loss[0, 0]


def solution(mesh):
    in_specs = (
        P("beam", "row", "col"),
        P("beam", "row", "col"),
        P(),
        P("row", "col", "beam", None, None),
        P("row", "col", "beam"),
        P("row", "col", "beam"),
    )
    out_specs = (P(None, "row", "col"), P(), P())
    return jax.shard_map(local, mesh=mesh, in_specs=in_specs, out_specs=out_specs, check_vma=False)
```

```python
import functools
import math

import jax
import jax.numpy as jnp
import numpy as np
from jax import lax
from jax.experimental import pallas as pl
from jax.experimental.pallas import tpu as pltpu
from jax.sharding import PartitionSpec as P

LANES = 128
SUBS = 8
CHUNK = 32
TOGETHER = 8
VMEM = pl.BlockSpec(memory_space=pltpu.VMEM)
SMEM = pl.BlockSpec(memory_space=pltpu.SMEM)
HBM = pl.BlockSpec(memory_space=pltpu.HBM)
F32 = jnp.float32
BF16 = jnp.bfloat16


def dft_blocks(length):
    indices = np.arange(length, dtype=np.int64)
    product = (indices[:, None] * indices[None, :] % length).astype(np.float32)
    angles = (product * np.float32(2.0 * math.pi / length)).astype(np.float64)
    factor = np.float32(1.0 / math.sqrt(length))
    real = (np.cos(angles).astype(np.float32) * factor).astype(jnp.bfloat16)
    imag = (-np.sin(angles).astype(np.float32) * factor).astype(jnp.bfloat16)
    forward = np.block([[real, -imag], [imag, real]])
    backward = np.block([[real, imag], [-imag, real]])
    return forward.astype(jnp.bfloat16), backward.astype(jnp.bfloat16)


def exchange(value, axis, mask):
    count = lax.axis_size(axis)
    return lax.ppermute(value, axis, [(i, i ^ mask) for i in range(count)])


def collected(own, values):
    far_first = {k: exchange(values[k], "beam", k) for k in reversed(range(1, len(values)))}
    return butterfly([own] + [far_first[k] for k in sorted(far_first)])


def butterfly(values):
    while len(values) > 1:
        values = [values[i] + values[i + 1] for i in range(0, len(values), 2)]
    return values[0]


def rows_of(index, size):
    return pl.ds(pl.multiple_of(index * size, size), size)


def sum_kernel(beams, phase_ref, absorb_ref, *refs):
    outs, (phase_now, absorb_now, sums, sems) = refs[:beams], refs[beams:]
    part = phase_now.shape[1] // beams
    copies = []
    for q in range(beams):
        where = pl.ds(q * part, part)
        for comp, (a, b) in enumerate(((phase_ref, phase_now), (absorb_ref, absorb_now))):
            copy = pltpu.make_async_copy(
                a.at[:, where, :], b.at[:, where, :], sems.at[2 * q + comp]
            )
            copy.start()
            copies.append(copy)
    for q in range(beams):
        where = pl.ds(q * part, part)
        for comp, ref in enumerate((phase_now, absorb_now)):
            copies[2 * q + comp].wait()
            total = ref[0, where, :].astype(F32)
            for d in range(1, ref.shape[0]):
                total = total + ref[d, where, :].astype(F32)
            sums[q, comp] = total
    for k in range(beams):
        outs[k][...] = sums[jnp.bitwise_xor(lax.axis_index("beam"), k)]


def wave_kernel(beams, cols, count, length, *refs):
    spot_ref = refs[0]
    held = 2 * beams
    mid_refs, left_refs, right_refs = (refs[1 + i * held : 1 + (i + 1) * held] for i in range(3))
    refs = refs[1 + 3 * held :]
    probe_ref, amp_ref, forward_ref, backward_ref = refs[:4]
    sends = 1 if cols == 2 else 2
    outs = refs[4 : 5 + sends]
    cells, canvas, probe_sum, miss, trans, psi, half_wave, far, chi, back, near = refs[
        5 + sends : -2
    ]
    scan_ref, scan_sem = refs[-2:]
    fetch = pltpu.make_async_copy(spot_ref, scan_ref, scan_sem)
    fetch.start()
    part = mid_refs[0].shape[1]
    tall = cells.shape[2]
    together = trans.shape[0]
    beam, col = lax.axis_index("beam"), lax.axis_index("col")
    has_left, has_right = col > 0, col < cols - 1
    for k in range(beams):
        quarter = jnp.bitwise_xor(beam, k)
        spots = (quarter + beams // 2, lax.rem(quarter + 3 * beams // 2, 2 * beams))
        for which, at in enumerate(spots):
            where = rows_of(at, part)
            for comp in range(2):
                outside = 1.0 - comp
                source = which * beams + k
                cells[comp, 0, where, :] = jnp.where(has_left, left_refs[source][comp], outside)
                cells[comp, 1, where, :] = mid_refs[source][comp]
                cells[comp, 2, where, :] = jnp.where(has_right, right_refs[source][comp], outside)
    canvas[...] = jnp.zeros_like(canvas)
    probe_sum[...] = jnp.zeros_like(probe_sum)
    miss[...] = jnp.zeros_like(miss)
    lane = lax.broadcasted_iota(jnp.int32, (CHUNK, LANES), 1)
    chunks = length // CHUNK
    fetch.wait()

    def make_psi(s, u):
        row_at, col_at = scan_ref[s], scan_ref[count + s]
        back_shift = lax.rem(LANES - col_at, LANES)
        low = lane < LANES - col_at
        for i in range(chunks):
            here = pl.ds(i * CHUNK, CHUNK)
            there = pl.ds(row_at + i * CHUNK, CHUNK)
            pieces = []
            for comp in range(2):
                turned = [
                    pltpu.roll(cells[comp, j, there, :], back_shift, 1) for j in range(3)
                ]
                pieces.append([jnp.where(low, turned[j], turned[j + 1]) for j in range(2)])
            for j in range(2):
                lanes = pl.ds(j * LANES, LANES)
                real, imag = pieces[0][j], pieces[1][j]
                trans[u, 0, j, here, :] = real
                trans[u, 1, j, here, :] = imag
                probe_real = probe_ref[0, here, lanes]
                probe_imag = probe_ref[1, here, lanes]
                psi[u, here, lanes] = (probe_real * real - probe_imag * imag).astype(BF16)
                psi[u, pl.ds(length + i * CHUNK, CHUNK), lanes] = (
                    probe_real * imag + probe_imag * real
                ).astype(BF16)

    def left_product(table, source, target, u):
        result = jnp.dot(table[...], source[u], preferred_element_type=F32).astype(BF16)
        target[u, :, :length] = result[:length]
        target[u, :, length:] = result[length:]

    def right_product(source, table, target, u):
        target[u] = jnp.dot(source[u], table[...], preferred_element_type=F32)

    def make_chi(s, u):
        for i in range(chunks):
            here = pl.ds(i * CHUNK, CHUNK)
            real, imag = far[u, here, :length], far[u, here, length:]
            amplitude = amp_ref[s, here, :].astype(F32)
            power = real * real + imag * imag
            off = jnp.sqrt(power) - amplitude
            wide = off * off
            wide = wide[:, :LANES] + wide[:, LANES:]
            miss[...] += wide.reshape(CHUNK // SUBS, SUBS, LANES).sum(0)
            ratio = 1.0 - amplitude * lax.rsqrt(jnp.maximum(power, 0.25))
            chi[u, here, :] = (real * ratio).astype(BF16)
            chi[u, pl.ds(length + i * CHUNK, CHUNK), :] = (imag * ratio).astype(BF16)

    def scatter(s, u):
        row_at, col_at = scan_ref[s], scan_ref[count + s]
        high = lane >= col_at
        for i in range(chunks):
            here = pl.ds(i * CHUNK, CHUNK)
            there = pl.ds(row_at + i * CHUNK, CHUNK)
            turned = [[], []]
            for j in range(2):
                lanes = pl.ds(j * LANES, LANES)
                grad_real = near[u, here, lanes]
                grad_imag = near[u, here, pl.ds(length + j * LANES, LANES)]
                real, imag = trans[u, 0, j, here, :], trans[u, 1, j, here, :]
                probe_sum[0, j, here, :] += real * grad_real + imag * grad_imag
                probe_sum[1, j, here, :] += real * grad_imag - imag * grad_real
                probe_real = probe_ref[0, here, lanes]
                probe_imag = probe_ref[1, here, lanes]
                turned[0].append(
                    pltpu.roll(probe_real * grad_real + probe_imag * grad_imag, col_at, 1)
                )
                turned[1].append(
                    pltpu.roll(probe_real * grad_imag - probe_imag * grad_real, col_at, 1)
                )
            for comp in range(2):
                first, second = turned[comp]
                canvas[comp, 0, there, :] += jnp.where(high, first, 0.0)
                canvas[comp, 1, there, :] += jnp.where(high, second, first)
                canvas[comp, 2, there, :] += jnp.where(high, 0.0, second)

    def first(s, u):
        make_psi(s, u)
        left_product(forward_ref, psi, half_wave, u)

    def second(s, u):
        right_product(half_wave, backward_ref, far, u)

    def third(s, u):
        make_chi(s, u)
        left_product(backward_ref, chi, back, u)

    def fourth(s, u):
        right_product(back, forward_ref, near, u)

    stages = (first, second, third, fourth, scatter)

    def group(g, carry):
        for t in range(together + len(stages) - 1):
            for k in (1, 4, 3, 2, 0):
                if 0 <= t - k < together:
                    stages[k](g * together + t - k, t - k)
        return carry

    lax.fori_loop(0, count // together, group, 0)
    base = 2 * tall
    if cols == 2:
        tiles = (1, 2 * has_right.astype(jnp.int32))
        comps = ((col,), (1 - col,))
    else:
        tiles = (1, 0, 2)
        comps = ((0, 1), (), ())
    for out, tile, held in zip(outs, tiles, comps):
        for comp in range(2):
            out[pl.ds(comp * tall, tall), :] = canvas[comp, tile]
        for n, comp in enumerate(held):
            for j in range(2):
                out[pl.ds(base + (2 * n + j) * length, length), :] = probe_sum[comp, j]
        if held:
            out[pl.ds(base + 2 * len(held) * length, SUBS), :] = miss[...]


def split_kernel(beams, tall, length, *refs):
    beam = lax.axis_index("beam")
    ins, outs, edges = refs[: -2 * beams], refs[-2 * beams : -beams], refs[-beams:]
    part = tall // (2 * beams)
    strip = length // beams
    planes = (ins[0].shape[0] - 2 * tall - SUBS) // length

    def fetch(where):
        total = ins[0][where, :]
        for ref in ins[1:]:
            total = total + ref[where, :]
        return total

    for k in range(beams):
        quarter = jnp.bitwise_xor(beam, k)
        spots = (quarter + beams // 2, lax.rem(quarter + 3 * beams // 2, 2 * beams))
        for out, at in zip((outs[k], edges[k]), spots):
            for comp in range(2):
                where = pl.ds(pl.multiple_of(comp * tall + at * part, SUBS), part)
                out[pl.ds(comp * part, part), :] = fetch(where)
        for n in range(planes):
            start = 2 * tall + n * length + quarter * strip
            where = pl.ds(pl.multiple_of(start, SUBS), strip)
            outs[k][pl.ds(2 * part + n * strip, strip), :] = fetch(where)
        where = pl.ds(2 * tall + planes * length, SUBS)
        outs[k][pl.ds(2 * part + planes * strip, SUBS), :] = fetch(where)


def final_kernel(beams, halves, planes, part, scale, total, *refs):
    beam, col = lax.axis_index("beam"), lax.axis_index("col")
    gathered = refs[:beams]
    if halves == 2:
        probes = [gathered, refs[beams : 2 * beams]]
    else:
        probes = [gathered]
    object_ref, probe_ref, loss_ref = refs[-3:]
    strip = (gathered[0].shape[0] - 2 * SUBS - 2 * part) // planes
    length = strip * beams
    miss_at = pl.ds(planes * strip, SUBS)
    square_at = pl.ds(planes * strip + SUBS, SUBS)
    for k in range(beams):
        quarter = jnp.bitwise_xor(beam, k)
        where = rows_of(quarter, strip)
        for h in range(halves):
            for n in range(planes):
                comp = (jnp.bitwise_xor(col, h)) if halves == 2 else n // 2
                lanes = pl.ds((n % 2) * LANES, LANES)
                probe_ref[comp, where, lanes] = (
                    probes[h][k][pl.ds(n * strip, strip), :] * (1.0 / total)
                )
    if halves == 2:
        squares = butterfly([ref[square_at, :] for ref in probes[0]])
        squares = squares + butterfly([ref[square_at, :] for ref in probes[1]])
    else:
        squares = refs[beams][...]
    mean_square = jnp.sum(squares, keepdims=True) * scale
    factor = jnp.minimum(1.0, 0.5 / jnp.sqrt(mean_square + 1e-06))
    loss = jnp.sum(gathered[0][miss_at, :], keepdims=True) / (total * length * length)
    loss_ref[...] = jnp.broadcast_to(loss, loss_ref.shape)
    base = planes * strip + 2 * SUBS
    for k in range(beams):
        where = rows_of(jnp.bitwise_xor(beam, k), part)
        for comp in range(2):
            object_ref[comp, where, :] = gathered[k][pl.ds(base + comp * part, part), :] * factor


def call(kernel, shapes, scalars, arrays, scratch=(), flops=0, array_spec=VMEM, limit=40 * 2**20):
    size = sum(a.size * a.dtype.itemsize for a in arrays)
    return pl.pallas_call(
        kernel,
        out_shape=[jax.ShapeDtypeStruct(s, F32) for s in shapes],
        in_specs=[SMEM] * len(scalars) + [array_spec] * len(arrays),
        out_specs=[VMEM] * len(shapes),
        scratch_shapes=list(scratch),
        compiler_params=pltpu.CompilerParams(vmem_limit_bytes=limit),
        cost_estimate=pl.CostEstimate(flops=flops, bytes_accessed=size, transcendentals=0),
    )(*scalars, *arrays)


def wave_call(sizes, scalars, arrays):
    beams, cols, count, length, tall = sizes
    paired = cols == 2
    deep = 2 * tall + (2 if paired else 4) * length + SUBS
    shapes = [(deep, LANES)] * 2 if paired else [(deep, LANES)] + [(2 * tall, LANES)] * 2
    u = math.gcd(count, TOGETHER)
    return call(
        functools.partial(wave_kernel, beams, cols, count, length),
        shapes,
        scalars,
        arrays + [jnp.asarray(table) for table in dft_blocks(length)],
        [
            pltpu.VMEM((2, 3, tall, LANES), F32),
            pltpu.VMEM((2, 3, tall, LANES), F32),
            pltpu.VMEM((2, 2, length, LANES), F32),
            pltpu.VMEM((SUBS, LANES), F32),
            pltpu.VMEM((u, 2, 2, length, LANES), F32),
            pltpu.VMEM((u, 2 * length, length), BF16),
            pltpu.VMEM((u, length, 2 * length), BF16),
            pltpu.VMEM((u, length, 2 * length), F32),
            pltpu.VMEM((u, 2 * length, length), BF16),
            pltpu.VMEM((u, length, 2 * length), BF16),
            pltpu.VMEM((u, length, 2 * length), F32),
            pltpu.SMEM((2 * count,), jnp.int32),
            pltpu.SemaphoreType.DMA,
        ],
        flops=count * 32 * length**3,
    )


def local(phase_volume, absorb_volume, probe, amplitudes, scan_rows, scan_cols):
    length = probe.shape[1]
    count = scan_rows.shape[2]
    rows_local = phase_volume.shape[1]
    cols_local = phase_volume.shape[2]
    beams, rows, cols = (lax.axis_size(a) for a in ("beam", "row", "col"))
    assert cols_local == LANES and length == 2 * LANES and rows_local == length
    places = jnp.concatenate([scan_rows.reshape(count), scan_cols.reshape(count)])
    part = rows_local // beams
    tall = rows_local + length
    others = range(1, beams)
    near_half = beams // 2

    def toward(value, step):
        pairs = []
        for b in range(beams):
            way = step if b >= near_half else -step
            for r in range(rows):
                if 0 <= r + way < rows:
                    pairs.append((b * rows + r, b * rows + r + way))
        return lax.ppermute(value, ("beam", "row"), pairs)

    sums = call(
        functools.partial(sum_kernel, beams),
        [(2, part, LANES)] * beams,
        [],
        [pltpu.with_memory_space_constraint(x, pltpu.HBM) for x in (phase_volume, absorb_volume)],
        [
            pltpu.VMEM(phase_volume.shape, BF16),
            pltpu.VMEM(phase_volume.shape, BF16),
            pltpu.VMEM((beams, 2, part, LANES), F32),
            pltpu.SemaphoreType.DMA((2 * beams,)),
        ],
        array_spec=HBM,
    )
    total, places = lax.optimization_barrier((collected(sums[0], sums), places))
    near = toward(total, 1)

    def spread(values):
        damping = jnp.exp(-values[1])
        wave = jnp.stack([damping * jnp.cos(values[0]), damping * jnp.sin(values[0])])
        return wave, [wave] + [exchange(wave, "beam", k) for k in others]

    trans, mids = spread(total)
    mids = mids + spread(near)[1]
    if cols == 2:
        lefts = [exchange(x, "col", 1) for x in mids]
        rights = lefts
    else:
        lefts = [lax.ppermute(x, "col", [(i, i + 1) for i in range(cols - 1)]) for x in mids]
        rights = [lax.ppermute(x, "col", [(i + 1, i) for i in range(cols - 1)]) for x in mids]
    paired = cols == 2
    planes = 2 if paired else 4
    outs = wave_call(
        (beams, cols, count, length, tall),
        [],
        [places, *mids, *lefts, *rights, probe, amplitudes.reshape(count, length, length)],
    )
    if paired:
        pieces = [outs[0], exchange(outs[1], "col", 1)]
    else:
        keep, to_left, to_right = outs
        edge = lax.ppermute(to_left, "col", [(i + 1, i) for i in range(cols - 1)])
        edge = edge + lax.ppermute(to_right, "col", [(i, i + 1) for i in range(cols - 1)])
        rest = lax.psum(keep[2 * tall :], "col")
        pieces = [jnp.concatenate([keep[: 2 * tall] + edge, rest])]
    strip = length // beams
    flat = 2 * part + planes * strip + SUBS
    split = call(
        functools.partial(split_kernel, beams, tall, length),
        [(flat, LANES)] * beams + [(2 * part, LANES)] * beams,
        [],
        pieces,
    )

    edge = toward(collected(split[beams], split[beams:]), -1)
    summed = collected(split[0], split[:beams])
    whole = summed[: 2 * part] + edge
    real, imag = whole[:part], whole[part:]
    grad_phase = trans[0] * imag - trans[1] * real
    grad_absorb = -(trans[0] * real + trans[1] * imag)
    squares = grad_phase * grad_phase + grad_absorb * grad_absorb
    squares = squares.reshape(part // SUBS, SUBS, LANES).sum(0)
    carried = jnp.concatenate([summed[2 * part :], squares])
    gradient = jnp.concatenate([grad_phase, grad_absorb])
    carried = butterfly(
        [carried] + [exchange(carried, "row", k) for k in range(1, rows)]
    )
    carried = jnp.concatenate([carried, gradient])
    gathered = [carried] + [exchange(carried, "beam", k) for k in others]
    at = planes * strip + SUBS
    if paired:
        more = [exchange(x[: at + SUBS], "col", 1) for x in gathered]
    else:
        more = [lax.psum(butterfly([x[at : at + SUBS] for x in gathered]), "col")]
    operands = gathered + more
    plane_devices = rows * cols
    objects_step, probe_gradient, loss = call(
        functools.partial(
            final_kernel,
            beams,
            2 if paired else 1,
            planes,
            part,
            1.0 / (2 * rows_local * cols_local * plane_devices),
            float(plane_devices * beams * count),
        ),
        [(2, rows_local, cols_local), (2, length, length), (1, 1)],
        [],
        operands,
    )
    return objects_step, probe_gradient, loss[0, 0]


def solution(mesh):
    in_specs = (
        P("beam", "row", "col"),
        P("beam", "row", "col"),
        P(),
        P("row", "col", "beam", None, None),
        P("row", "col", "beam"),
        P("row", "col", "beam"),
    )
    out_specs = (P(None, "row", "col"), P(), P())
    return jax.shard_map(local, mesh=mesh, in_specs=in_specs, out_specs=out_specs, check_vma=False)
```

```python
import functools
import math

import jax
import jax.numpy as jnp
import numpy as np
from jax import lax
from jax.experimental import pallas as pl
from jax.experimental.pallas import tpu as pltpu
from jax.sharding import PartitionSpec as P

LANES = 128
SUBS = 8
CHUNK = 32
TOGETHER = 8
VMEM = pl.BlockSpec(memory_space=pltpu.VMEM)
SMEM = pl.BlockSpec(memory_space=pltpu.SMEM)
HBM = pl.BlockSpec(memory_space=pltpu.HBM)
F32 = jnp.float32
BF16 = jnp.bfloat16


def dft_blocks(length):
    indices = np.arange(length, dtype=np.int64)
    product = (indices[:, None] * indices[None, :] % length).astype(np.float32)
    angles = (product * np.float32(2.0 * math.pi / length)).astype(np.float64)
    factor = np.float32(1.0 / math.sqrt(length))
    real = (np.cos(angles).astype(np.float32) * factor).astype(jnp.bfloat16)
    imag = (-np.sin(angles).astype(np.float32) * factor).astype(jnp.bfloat16)
    forward = np.block([[real, -imag], [imag, real]])
    backward = np.block([[real, imag], [-imag, real]])
    return forward.astype(jnp.bfloat16), backward.astype(jnp.bfloat16)


def exchange(value, axis, mask):
    count = lax.axis_size(axis)
    return lax.ppermute(value, axis, [(i, i ^ mask) for i in range(count)])


def my_quarter(beams):
    even = 1 - lax.rem(lax.axis_index("row"), 2)
    return jnp.bitwise_xor(lax.axis_index("beam"), even * (beams // 2))


def spots_of(quarter, beams):
    across = jnp.bitwise_xor(quarter, beams // 2)
    return quarter + beams // 2, lax.rem(across + 3 * beams // 2, 2 * beams)


def collected(own, values):
    far_first = {k: exchange(values[k], "beam", k) for k in reversed(range(1, len(values)))}
    return butterfly([own] + [far_first[k] for k in sorted(far_first)])


def butterfly(values):
    while len(values) > 1:
        values = [values[i] + values[i + 1] for i in range(0, len(values), 2)]
    return values[0]


def rows_of(index, size):
    return pl.ds(pl.multiple_of(index * size, size), size)


def sum_kernel(beams, phase_ref, absorb_ref, *refs):
    outs, (phase_now, absorb_now, sums, sems) = refs[:beams], refs[beams:]
    part = phase_now.shape[1] // beams
    copies = []
    for q in range(beams):
        where = pl.ds(q * part, part)
        for comp, (a, b) in enumerate(((phase_ref, phase_now), (absorb_ref, absorb_now))):
            copy = pltpu.make_async_copy(
                a.at[:, where, :], b.at[:, where, :], sems.at[2 * q + comp]
            )
            copy.start()
            copies.append(copy)
    for q in range(beams):
        where = pl.ds(q * part, part)
        for comp, ref in enumerate((phase_now, absorb_now)):
            copies[2 * q + comp].wait()
            total = ref[0, where, :].astype(F32)
            for d in range(1, ref.shape[0]):
                total = total + ref[d, where, :].astype(F32)
            sums[q, comp] = total
    for k in range(beams):
        outs[k][...] = sums[jnp.bitwise_xor(my_quarter(beams), k)]


def wave_kernel(beams, cols, count, length, *refs):
    spot_ref = refs[0]
    held = 2 * beams
    mid_refs, left_refs, right_refs = (refs[1 + i * held : 1 + (i + 1) * held] for i in range(3))
    refs = refs[1 + 3 * held :]
    probe_ref, amp_ref, forward_ref, backward_ref = refs[:4]
    sends = 1 if cols == 2 else 2
    outs = refs[4 : 5 + sends]
    cells, canvas, probe_sum, miss, trans, psi, half_wave, far, chi, back, near = refs[
        5 + sends : -2
    ]
    scan_ref, scan_sem = refs[-2:]
    fetch = pltpu.make_async_copy(spot_ref, scan_ref, scan_sem)
    fetch.start()
    part = mid_refs[0].shape[1]
    tall = cells.shape[2]
    together = trans.shape[0]
    beam, col = my_quarter(beams), lax.axis_index("col")
    has_left, has_right = col > 0, col < cols - 1
    for k in range(beams):
        quarter = jnp.bitwise_xor(beam, k)
        spots = spots_of(quarter, beams)
        for which, at in enumerate(spots):
            where = rows_of(at, part)
            for comp in range(2):
                outside = 1.0 - comp
                source = which * beams + k
                cells[comp, 0, where, :] = jnp.where(has_left, left_refs[source][comp], outside)
                cells[comp, 1, where, :] = mid_refs[source][comp]
                cells[comp, 2, where, :] = jnp.where(has_right, right_refs[source][comp], outside)
    canvas[...] = jnp.zeros_like(canvas)
    probe_sum[...] = jnp.zeros_like(probe_sum)
    miss[...] = jnp.zeros_like(miss)
    lane = lax.broadcasted_iota(jnp.int32, (CHUNK, LANES), 1)
    chunks = length // CHUNK
    fetch.wait()

    def make_psi(s, u):
        row_at, col_at = scan_ref[s], scan_ref[count + s]
        back_shift = lax.rem(LANES - col_at, LANES)
        low = lane < LANES - col_at
        for i in range(chunks):
            here = pl.ds(i * CHUNK, CHUNK)
            there = pl.ds(row_at + i * CHUNK, CHUNK)
            pieces = []
            for comp in range(2):
                turned = [
                    pltpu.roll(cells[comp, j, there, :], back_shift, 1) for j in range(3)
                ]
                pieces.append([jnp.where(low, turned[j], turned[j + 1]) for j in range(2)])
            for j in range(2):
                lanes = pl.ds(j * LANES, LANES)
                real, imag = pieces[0][j], pieces[1][j]
                trans[u, 0, j, here, :] = real
                trans[u, 1, j, here, :] = imag
                probe_real = probe_ref[0, here, lanes]
                probe_imag = probe_ref[1, here, lanes]
                psi[u, here, lanes] = (probe_real * real - probe_imag * imag).astype(BF16)
                psi[u, pl.ds(length + i * CHUNK, CHUNK), lanes] = (
                    probe_real * imag + probe_imag * real
                ).astype(BF16)

    def left_product(table, source, target, u):
        result = jnp.dot(table[...], source[u], preferred_element_type=F32).astype(BF16)
        target[u, :, :length] = result[:length]
        target[u, :, length:] = result[length:]

    def right_product(source, table, target, u):
        target[u] = jnp.dot(source[u], table[...], preferred_element_type=F32)

    def make_chi(s, u):
        for i in range(chunks):
            here = pl.ds(i * CHUNK, CHUNK)
            real, imag = far[u, here, :length], far[u, here, length:]
            amplitude = amp_ref[s, here, :].astype(F32)
            power = real * real + imag * imag
            off = jnp.sqrt(power) - amplitude
            wide = off * off
            wide = wide[:, :LANES] + wide[:, LANES:]
            miss[...] += wide.reshape(CHUNK // SUBS, SUBS, LANES).sum(0)
            ratio = 1.0 - amplitude * lax.rsqrt(jnp.maximum(power, 0.25))
            chi[u, here, :] = (real * ratio).astype(BF16)
            chi[u, pl.ds(length + i * CHUNK, CHUNK), :] = (imag * ratio).astype(BF16)

    def scatter(s, u):
        row_at, col_at = scan_ref[s], scan_ref[count + s]
        high = lane >= col_at
        for i in range(chunks):
            here = pl.ds(i * CHUNK, CHUNK)
            there = pl.ds(row_at + i * CHUNK, CHUNK)
            turned = [[], []]
            for j in range(2):
                lanes = pl.ds(j * LANES, LANES)
                grad_real = near[u, here, lanes]
                grad_imag = near[u, here, pl.ds(length + j * LANES, LANES)]
                real, imag = trans[u, 0, j, here, :], trans[u, 1, j, here, :]
                probe_sum[0, j, here, :] += real * grad_real + imag * grad_imag
                probe_sum[1, j, here, :] += real * grad_imag - imag * grad_real
                probe_real = probe_ref[0, here, lanes]
                probe_imag = probe_ref[1, here, lanes]
                turned[0].append(
                    pltpu.roll(probe_real * grad_real + probe_imag * grad_imag, col_at, 1)
                )
                turned[1].append(
                    pltpu.roll(probe_real * grad_imag - probe_imag * grad_real, col_at, 1)
                )
            for comp in range(2):
                first, second = turned[comp]
                canvas[comp, 0, there, :] += jnp.where(high, first, 0.0)
                canvas[comp, 1, there, :] += jnp.where(high, second, first)
                canvas[comp, 2, there, :] += jnp.where(high, 0.0, second)

    def first(s, u):
        make_psi(s, u)
        left_product(forward_ref, psi, half_wave, u)

    def second(s, u):
        right_product(half_wave, backward_ref, far, u)

    def third(s, u):
        make_chi(s, u)
        left_product(backward_ref, chi, back, u)

    def fourth(s, u):
        right_product(back, forward_ref, near, u)

    stages = (first, second, third, fourth, scatter)

    def group(g, carry):
        for t in range(together + len(stages) - 1):
            for k in (1, 4, 3, 2, 0):
                if 0 <= t - k < together:
                    stages[k](g * together + t - k, t - k)
        return carry

    lax.fori_loop(0, count // together, group, 0)
    base = 2 * tall
    if cols == 2:
        tiles = (1, 2 * has_right.astype(jnp.int32))
        comps = ((col,), (1 - col,))
    else:
        tiles = (1, 0, 2)
        comps = ((0, 1), (), ())
    for out, tile, held in zip(outs, tiles, comps):
        for comp in range(2):
            out[pl.ds(comp * tall, tall), :] = canvas[comp, tile]
        for n, comp in enumerate(held):
            for j in range(2):
                out[pl.ds(base + (2 * n + j) * length, length), :] = probe_sum[comp, j]
        if held:
            out[pl.ds(base + 2 * len(held) * length, SUBS), :] = miss[...]


def split_kernel(beams, tall, length, *refs):
    beam = my_quarter(beams)
    ins, outs, edges = refs[: -2 * beams], refs[-2 * beams : -beams], refs[-beams:]
    part = tall // (2 * beams)
    strip = length // beams
    planes = (ins[0].shape[0] - 2 * tall - SUBS) // length

    def fetch(where):
        total = ins[0][where, :]
        for ref in ins[1:]:
            total = total + ref[where, :]
        return total

    for k in range(beams):
        quarter = jnp.bitwise_xor(beam, k)
        spots = spots_of(quarter, beams)
        for out, at in zip((outs[k], edges[k]), spots):
            for comp in range(2):
                where = pl.ds(pl.multiple_of(comp * tall + at * part, SUBS), part)
                out[pl.ds(comp * part, part), :] = fetch(where)
        band = jnp.bitwise_xor(lax.axis_index("beam"), k)
        for n in range(planes):
            start = 2 * tall + n * length + band * strip
            where = pl.ds(pl.multiple_of(start, SUBS), strip)
            edges[k][pl.ds(2 * part + n * strip, strip), :] = fetch(where)
        where = pl.ds(2 * tall + planes * length, SUBS)
        edges[k][pl.ds(2 * part + planes * strip, SUBS), :] = fetch(where)


def final_kernel(beams, halves, planes, part, scale, total, *refs):
    beam, col = my_quarter(beams), lax.axis_index("col")
    gathered = refs[:beams]
    if halves == 2:
        probes = [gathered, refs[beams : 2 * beams]]
    else:
        probes = [gathered]
    object_ref, probe_ref, loss_ref = refs[-3:]
    strip = (gathered[0].shape[0] - 2 * SUBS - 2 * part) // planes
    length = strip * beams
    miss_at = pl.ds(planes * strip, SUBS)
    square_at = pl.ds(planes * strip + SUBS, SUBS)
    for k in range(beams):
        band = jnp.bitwise_xor(lax.axis_index("beam"), k)
        where = rows_of(band, strip)
        for h in range(halves):
            for n in range(planes):
                comp = (jnp.bitwise_xor(col, h)) if halves == 2 else n // 2
                lanes = pl.ds((n % 2) * LANES, LANES)
                probe_ref[comp, where, lanes] = (
                    probes[h][k][pl.ds(n * strip, strip), :] * (1.0 / total)
                )
    if halves == 2:
        squares = butterfly([ref[square_at, :] for ref in probes[0]])
        squares = squares + butterfly([ref[square_at, :] for ref in probes[1]])
    else:
        squares = refs[beams][...]
    mean_square = jnp.sum(squares, keepdims=True) * scale
    factor = jnp.minimum(1.0, 0.5 / jnp.sqrt(mean_square + 1e-06))
    misses = butterfly([ref[miss_at, :] for ref in gathered])
    loss = jnp.sum(misses, keepdims=True) / (beams * total * length * length)
    loss_ref[...] = jnp.broadcast_to(loss, loss_ref.shape)
    base = planes * strip + 2 * SUBS
    for k in range(beams):
        where = rows_of(jnp.bitwise_xor(beam, k), part)
        for comp in range(2):
            object_ref[comp, where, :] = gathered[k][pl.ds(base + comp * part, part), :] * factor


def call(kernel, shapes, scalars, arrays, scratch=(), flops=0, array_spec=VMEM, limit=40 * 2**20):
    size = sum(a.size * a.dtype.itemsize for a in arrays)
    return pl.pallas_call(
        kernel,
        out_shape=[jax.ShapeDtypeStruct(s, F32) for s in shapes],
        in_specs=[SMEM] * len(scalars) + [array_spec] * len(arrays),
        out_specs=[VMEM] * len(shapes),
        scratch_shapes=list(scratch),
        compiler_params=pltpu.CompilerParams(vmem_limit_bytes=limit),
        cost_estimate=pl.CostEstimate(flops=flops, bytes_accessed=size, transcendentals=0),
    )(*scalars, *arrays)


def wave_call(sizes, scalars, arrays):
    beams, cols, count, length, tall = sizes
    paired = cols == 2
    deep = 2 * tall + (2 if paired else 4) * length + SUBS
    shapes = [(deep, LANES)] * 2 if paired else [(deep, LANES)] + [(2 * tall, LANES)] * 2
    u = math.gcd(count, TOGETHER)
    return call(
        functools.partial(wave_kernel, beams, cols, count, length),
        shapes,
        scalars,
        arrays + [jnp.asarray(table) for table in dft_blocks(length)],
        [
            pltpu.VMEM((2, 3, tall, LANES), F32),
            pltpu.VMEM((2, 3, tall, LANES), F32),
            pltpu.VMEM((2, 2, length, LANES), F32),
            pltpu.VMEM((SUBS, LANES), F32),
            pltpu.VMEM((u, 2, 2, length, LANES), F32),
            pltpu.VMEM((u, 2 * length, length), BF16),
            pltpu.VMEM((u, length, 2 * length), BF16),
            pltpu.VMEM((u, length, 2 * length), F32),
            pltpu.VMEM((u, 2 * length, length), BF16),
            pltpu.VMEM((u, length, 2 * length), BF16),
            pltpu.VMEM((u, length, 2 * length), F32),
            pltpu.SMEM((2 * count,), jnp.int32),
            pltpu.SemaphoreType.DMA,
        ],
        flops=count * 32 * length**3,
    )


def local(phase_volume, absorb_volume, probe, amplitudes, scan_rows, scan_cols):
    length = probe.shape[1]
    count = scan_rows.shape[2]
    rows_local = phase_volume.shape[1]
    cols_local = phase_volume.shape[2]
    beams, rows, cols = (lax.axis_size(a) for a in ("beam", "row", "col"))
    assert cols_local == LANES and length == 2 * LANES and rows_local == length
    places = jnp.concatenate([scan_rows.reshape(count), scan_cols.reshape(count)])
    part = rows_local // beams
    tall = rows_local + length
    others = range(1, beams)
    near_half = beams // 2

    def swapped(value):
        pairs = []
        for b in range(beams):
            for r in range(rows):
                mate = r ^ 1 if b < near_half else (((r + 1) ^ 1) - 1) % rows
                pairs.append((b * rows + r, b * rows + mate))
        return lax.ppermute(value, ("beam", "row"), pairs)

    beam, row = lax.axis_index("beam"), lax.axis_index("row")
    inside = (beam < near_half) | ((row > 0) & (row < rows - 1))

    sums = call(
        functools.partial(sum_kernel, beams),
        [(2, part, LANES)] * beams,
        [],
        [pltpu.with_memory_space_constraint(x, pltpu.HBM) for x in (phase_volume, absorb_volume)],
        [
            pltpu.VMEM(phase_volume.shape, BF16),
            pltpu.VMEM(phase_volume.shape, BF16),
            pltpu.VMEM((beams, 2, part, LANES), F32),
            pltpu.SemaphoreType.DMA((2 * beams,)),
        ],
        array_spec=HBM,
    )
    sums, amplitudes, probe = lax.optimization_barrier((list(sums), amplitudes, probe))
    total, places = lax.optimization_barrier((collected(sums[0], sums), places))
    near = jnp.where(inside, swapped(total), 0.0)

    def spread(values):
        damping = jnp.exp(-values[1])
        wave = jnp.stack([damping * jnp.cos(values[0]), damping * jnp.sin(values[0])])
        return wave, [wave] + [exchange(wave, "beam", k) for k in others]

    trans, mids = spread(total)
    mids = mids + spread(near)[1]
    if cols == 2:
        lefts = [exchange(x, "col", 1) for x in mids]
        rights = lefts
    else:
        lefts = [lax.ppermute(x, "col", [(i, i + 1) for i in range(cols - 1)]) for x in mids]
        rights = [lax.ppermute(x, "col", [(i + 1, i) for i in range(cols - 1)]) for x in mids]
    paired = cols == 2
    planes = 2 if paired else 4
    outs = wave_call(
        (beams, cols, count, length, tall),
        [],
        [places, *mids, *lefts, *rights, probe, amplitudes.reshape(count, length, length)],
    )
    if paired:
        pieces = [outs[0], exchange(outs[1], "col", 1)]
    else:
        keep, to_left, to_right = outs
        edge = lax.ppermute(to_left, "col", [(i + 1, i) for i in range(cols - 1)])
        edge = edge + lax.ppermute(to_right, "col", [(i, i + 1) for i in range(cols - 1)])
        rest = lax.psum(keep[2 * tall :], "col")
        pieces = [jnp.concatenate([keep[: 2 * tall] + edge, rest])]
    strip = length // beams
    flat = 2 * part + planes * strip + SUBS
    split = call(
        functools.partial(split_kernel, beams, tall, length),
        [(2 * part, LANES)] * beams + [(flat, LANES)] * beams,
        [],
        pieces,
    )

    outer = collected(split[beams], split[beams:])
    crossed = swapped(outer)
    whole = collected(split[0], split[:beams])
    whole = whole + jnp.where(inside, crossed[: 2 * part], 0.0)
    terms = outer[2 * part :] + crossed[2 * part :]
    real, imag = whole[:part], whole[part:]
    grad_phase = trans[0] * imag - trans[1] * real
    grad_absorb = -(trans[0] * real + trans[1] * imag)
    squares = grad_phase * grad_phase + grad_absorb * grad_absorb
    squares = squares.reshape(part // SUBS, SUBS, LANES).sum(0)
    gradient = jnp.concatenate([grad_phase, grad_absorb])
    moving = jnp.concatenate([terms, squares])
    shifts = {
        k: lax.ppermute(
            squares if k % 2 else moving, "row", [(i, (i + k) % rows) for i in range(rows)]
        )
        for k in range(1, rows)
    }
    at = planes * strip + SUBS
    for k in range(2, rows, 2):
        terms = terms + shifts[k][:at]
    each = {k: shifts[k] if k % 2 else shifts[k][at:] for k in shifts}
    evens = [squares] + [each[k] for k in range(2, rows, 2)]
    odds = [each[k] for k in range(1, rows, 2)]
    squares = functools.reduce(jnp.add, evens) + functools.reduce(jnp.add, odds)
    carried = jnp.concatenate([terms, squares, gradient])
    gathered = [carried] + [exchange(carried, "beam", k) for k in others]
    if paired:
        more = [exchange(x[: at + SUBS], "col", 1) for x in gathered]
    else:
        more = [lax.psum(butterfly([x[at : at + SUBS] for x in gathered]), "col")]
    operands = gathered + more
    plane_devices = rows * cols
    objects_step, probe_gradient, loss = call(
        functools.partial(
            final_kernel,
            beams,
            2 if paired else 1,
            planes,
            part,
            1.0 / (2 * rows_local * cols_local * plane_devices),
            float(plane_devices * beams * count),
        ),
        [(2, rows_local, cols_local), (2, length, length), (1, 1)],
        [],
        operands,
    )
    return objects_step, probe_gradient, loss[0, 0]


def solution(mesh):
    in_specs = (
        P("beam", "row", "col"),
        P("beam", "row", "col"),
        P(),
        P("row", "col", "beam", None, None),
        P("row", "col", "beam"),
        P("row", "col", "beam"),
    )
    out_specs = (P(None, "row", "col"), P(), P())
    return jax.shard_map(local, mesh=mesh, in_specs=in_specs, out_specs=out_specs, check_vma=False)
```

```python
import functools
import math

import jax
import jax.numpy as jnp
import numpy as np
from jax import lax
from jax.experimental import pallas as pl
from jax.experimental.pallas import tpu as pltpu
from jax.sharding import PartitionSpec as P

LANES = 128
SUBS = 8
CHUNK = 32
TOGETHER = 8
VMEM = pl.BlockSpec(memory_space=pltpu.VMEM)
SMEM = pl.BlockSpec(memory_space=pltpu.SMEM)
HBM = pl.BlockSpec(memory_space=pltpu.HBM)
F32 = jnp.float32
BF16 = jnp.bfloat16


def dft_blocks(length):
    indices = np.arange(length, dtype=np.int64)
    product = (indices[:, None] * indices[None, :] % length).astype(np.float32)
    angles = (product * np.float32(2.0 * math.pi / length)).astype(np.float64)
    factor = np.float32(1.0 / math.sqrt(length))
    real = (np.cos(angles).astype(np.float32) * factor).astype(jnp.bfloat16)
    imag = (-np.sin(angles).astype(np.float32) * factor).astype(jnp.bfloat16)
    forward = np.block([[real, -imag], [imag, real]])
    backward = np.block([[real, imag], [-imag, real]])
    return forward.astype(jnp.bfloat16), backward.astype(jnp.bfloat16)


def exchange(value, axis, mask):
    count = lax.axis_size(axis)
    return lax.ppermute(value, axis, [(i, i ^ mask) for i in range(count)])


def my_quarter(beams):
    even = 1 - lax.rem(lax.axis_index("row"), 2)
    return jnp.bitwise_xor(lax.axis_index("beam"), even * (beams // 2))


def spots_of(quarter, beams):
    across = jnp.bitwise_xor(quarter, beams // 2)
    return quarter + beams // 2, lax.rem(across + 3 * beams // 2, 2 * beams)


def collected(own, values):
    far_first = {k: exchange(values[k], "beam", k) for k in reversed(range(1, len(values)))}
    return butterfly([own] + [far_first[k] for k in sorted(far_first)])


def butterfly(values):
    while len(values) > 1:
        values = [values[i] + values[i + 1] for i in range(0, len(values), 2)]
    return values[0]


def rows_of(index, size):
    return pl.ds(pl.multiple_of(index * size, size), size)


def sum_kernel(beams, phase_ref, absorb_ref, *refs):
    outs, (phase_now, absorb_now, sums, sems) = refs[:beams], refs[beams:]
    part = phase_now.shape[1] // beams
    copies = []
    for q in range(beams):
        where = pl.ds(q * part, part)
        for comp, (a, b) in enumerate(((phase_ref, phase_now), (absorb_ref, absorb_now))):
            copy = pltpu.make_async_copy(
                a.at[:, where, :], b.at[:, where, :], sems.at[2 * q + comp]
            )
            copy.start()
            copies.append(copy)
    for q in range(beams):
        where = pl.ds(q * part, part)
        for comp, ref in enumerate((phase_now, absorb_now)):
            copies[2 * q + comp].wait()
            total = ref[0, where, :].astype(F32)
            for d in range(1, ref.shape[0]):
                total = total + ref[d, where, :].astype(F32)
            sums[q, comp] = total
    for k in range(beams):
        outs[k][...] = sums[jnp.bitwise_xor(my_quarter(beams), k)]


def wave_kernel(beams, cols, count, length, *refs):
    spot_ref = refs[0]
    held = 2 * beams
    mid_refs, left_refs, right_refs = (refs[1 + i * held : 1 + (i + 1) * held] for i in range(3))
    refs = refs[1 + 3 * held :]
    probe_ref, amp_ref, forward_ref, backward_ref = refs[:4]
    sends = 1 if cols == 2 else 2
    outs = refs[4 : 5 + sends]
    cells, canvas, probe_sum, miss, trans, psi, half_wave, far, chi, back, near = refs[
        5 + sends : -2
    ]
    scan_ref, scan_sem = refs[-2:]
    fetch = pltpu.make_async_copy(spot_ref, scan_ref, scan_sem)
    fetch.start()
    part = mid_refs[0].shape[1]
    tall = cells.shape[2]
    together = trans.shape[0]
    beam, col = my_quarter(beams), lax.axis_index("col")
    has_left, has_right = col > 0, col < cols - 1
    for k in range(beams):
        quarter = jnp.bitwise_xor(beam, k)
        spots = spots_of(quarter, beams)
        for which, at in enumerate(spots):
            where = rows_of(at, part)
            for comp in range(2):
                outside = 1.0 - comp
                source = which * beams + k
                cells[comp, 0, where, :] = jnp.where(has_left, left_refs[source][comp], outside)
                cells[comp, 1, where, :] = mid_refs[source][comp]
                cells[comp, 2, where, :] = jnp.where(has_right, right_refs[source][comp], outside)
    canvas[...] = jnp.zeros_like(canvas)
    probe_sum[...] = jnp.zeros_like(probe_sum)
    miss[...] = jnp.zeros_like(miss)
    lane = lax.broadcasted_iota(jnp.int32, (CHUNK, LANES), 1)
    chunks = length // CHUNK
    fetch.wait()

    def make_psi(s, u):
        row_at, col_at = scan_ref[s], scan_ref[count + s]
        back_shift = lax.rem(LANES - col_at, LANES)
        low = lane < LANES - col_at
        for i in range(chunks):
            here = pl.ds(i * CHUNK, CHUNK)
            there = pl.ds(row_at + i * CHUNK, CHUNK)
            pieces = []
            for comp in range(2):
                turned = [
                    pltpu.roll(cells[comp, j, there, :], back_shift, 1) for j in range(3)
                ]
                pieces.append([jnp.where(low, turned[j], turned[j + 1]) for j in range(2)])
            for j in range(2):
                lanes = pl.ds(j * LANES, LANES)
                real, imag = pieces[0][j], pieces[1][j]
                trans[u, 0, j, here, :] = real
                trans[u, 1, j, here, :] = imag
                probe_real = probe_ref[0, here, lanes]
                probe_imag = probe_ref[1, here, lanes]
                psi[u, here, lanes] = (probe_real * real - probe_imag * imag).astype(BF16)
                psi[u, pl.ds(length + i * CHUNK, CHUNK), lanes] = (
                    probe_real * imag + probe_imag * real
                ).astype(BF16)

    def left_product(table, source, target, u):
        result = jnp.dot(table[...], source[u], preferred_element_type=F32).astype(BF16)
        target[u, :, :length] = result[:length]
        target[u, :, length:] = result[length:]

    def right_product(source, table, target, u):
        target[u] = jnp.dot(source[u], table[...], preferred_element_type=F32)

    def make_chi(s, u):
        for i in range(chunks):
            here = pl.ds(i * CHUNK, CHUNK)
            real, imag = far[u, here, :length], far[u, here, length:]
            amplitude = amp_ref[s, here, :].astype(F32)
            power = real * real + imag * imag
            off = jnp.sqrt(power) - amplitude
            wide = off * off
            wide = wide[:, :LANES] + wide[:, LANES:]
            miss[...] += wide.reshape(CHUNK // SUBS, SUBS, LANES).sum(0)
            ratio = 1.0 - amplitude * lax.rsqrt(jnp.maximum(power, 0.25))
            chi[u, here, :] = (real * ratio).astype(BF16)
            chi[u, pl.ds(length + i * CHUNK, CHUNK), :] = (imag * ratio).astype(BF16)

    def scatter(s, u):
        row_at, col_at = scan_ref[s], scan_ref[count + s]
        high = lane >= col_at
        for i in range(chunks):
            here = pl.ds(i * CHUNK, CHUNK)
            there = pl.ds(row_at + i * CHUNK, CHUNK)
            turned = [[], []]
            for j in range(2):
                lanes = pl.ds(j * LANES, LANES)
                grad_real = near[u, here, lanes]
                grad_imag = near[u, here, pl.ds(length + j * LANES, LANES)]
                real, imag = trans[u, 0, j, here, :], trans[u, 1, j, here, :]
                probe_sum[0, j, here, :] += real * grad_real + imag * grad_imag
                probe_sum[1, j, here, :] += real * grad_imag - imag * grad_real
                probe_real = probe_ref[0, here, lanes]
                probe_imag = probe_ref[1, here, lanes]
                turned[0].append(
                    pltpu.roll(probe_real * grad_real + probe_imag * grad_imag, col_at, 1)
                )
                turned[1].append(
                    pltpu.roll(probe_real * grad_imag - probe_imag * grad_real, col_at, 1)
                )
            for comp in range(2):
                first, second = turned[comp]
                canvas[comp, 0, there, :] += jnp.where(high, first, 0.0)
                canvas[comp, 1, there, :] += jnp.where(high, second, first)
                canvas[comp, 2, there, :] += jnp.where(high, 0.0, second)

    def first(s, u):
        make_psi(s, u)
        left_product(forward_ref, psi, half_wave, u)

    def second(s, u):
        right_product(half_wave, backward_ref, far, u)

    def third(s, u):
        make_chi(s, u)
        left_product(backward_ref, chi, back, u)

    def fourth(s, u):
        right_product(back, forward_ref, near, u)

    stages = (first, second, third, fourth, scatter)

    def group(g, carry):
        for t in range(together + len(stages) - 1):
            for k in (1, 4, 3, 2, 0):
                if 0 <= t - k < together:
                    stages[k](g * together + t - k, t - k)
        return carry

    lax.fori_loop(0, count // together, group, 0)
    base = 2 * tall
    if cols == 2:
        tiles = (1, 2 * has_right.astype(jnp.int32))
        comps = ((col,), (1 - col,))
    else:
        tiles = (1, 0, 2)
        comps = ((0, 1), (), ())
    for out, tile, held in zip(outs, tiles, comps):
        for comp in range(2):
            out[pl.ds(comp * tall, tall), :] = canvas[comp, tile]
        for n, comp in enumerate(held):
            for j in range(2):
                out[pl.ds(base + (2 * n + j) * length, length), :] = probe_sum[comp, j]
        if held:
            out[pl.ds(base + 2 * len(held) * length, SUBS), :] = miss[...]


def split_kernel(beams, tall, length, *refs):
    beam = my_quarter(beams)
    ins, outs, edges = refs[: -2 * beams], refs[-2 * beams : -beams], refs[-beams:]
    part = tall // (2 * beams)
    strip = length // beams
    planes = (ins[0].shape[0] - 2 * tall - SUBS) // length

    def fetch(where):
        total = ins[0][where, :]
        for ref in ins[1:]:
            total = total + ref[where, :]
        return total

    for k in range(beams):
        quarter = jnp.bitwise_xor(beam, k)
        spots = spots_of(quarter, beams)
        for out, at in zip((outs[k], edges[k]), spots):
            for comp in range(2):
                where = pl.ds(pl.multiple_of(comp * tall + at * part, SUBS), part)
                out[pl.ds(comp * part, part), :] = fetch(where)
        band = jnp.bitwise_xor(lax.axis_index("beam"), k)
        for n in range(planes):
            start = 2 * tall + n * length + band * strip
            where = pl.ds(pl.multiple_of(start, SUBS), strip)
            outs[k][pl.ds(2 * part + n * strip, strip), :] = fetch(where)
        where = pl.ds(2 * tall + planes * length, SUBS)
        outs[k][pl.ds(2 * part + planes * strip, SUBS), :] = fetch(where)


def final_kernel(beams, halves, planes, part, scale, total, *refs):
    beam, col = my_quarter(beams), lax.axis_index("col")
    gathered = refs[:beams]
    if halves == 2:
        probes = [gathered, refs[beams : 2 * beams]]
    else:
        probes = [gathered]
    object_ref, probe_ref, loss_ref = refs[-3:]
    strip = (gathered[0].shape[0] - 2 * SUBS - 2 * part) // planes
    length = strip * beams
    miss_at = pl.ds(planes * strip, SUBS)
    square_at = pl.ds(planes * strip + SUBS, SUBS)
    for k in range(beams):
        band = jnp.bitwise_xor(lax.axis_index("beam"), k)
        where = rows_of(band, strip)
        for h in range(halves):
            for n in range(planes):
                comp = (jnp.bitwise_xor(col, h)) if halves == 2 else n // 2
                lanes = pl.ds((n % 2) * LANES, LANES)
                probe_ref[comp, where, lanes] = (
                    probes[h][k][pl.ds(n * strip, strip), :] * (1.0 / total)
                )
    if halves == 2:
        squares = butterfly([ref[square_at, :] for ref in probes[0]])
        squares = squares + butterfly([ref[square_at, :] for ref in probes[1]])
    else:
        squares = refs[beams][...]
    mean_square = jnp.sum(squares, keepdims=True) * scale
    factor = jnp.minimum(1.0, 0.5 / jnp.sqrt(mean_square + 1e-06))
    misses = butterfly([ref[miss_at, :] for ref in gathered])
    loss = jnp.sum(misses, keepdims=True) / (beams * total * length * length)
    loss_ref[...] = jnp.broadcast_to(loss, loss_ref.shape)
    base = planes * strip + 2 * SUBS
    for k in range(beams):
        where = rows_of(jnp.bitwise_xor(beam, k), part)
        for comp in range(2):
            object_ref[comp, where, :] = gathered[k][pl.ds(base + comp * part, part), :] * factor


def call(kernel, shapes, scalars, arrays, scratch=(), flops=0, array_spec=VMEM, limit=40 * 2**20):
    size = sum(a.size * a.dtype.itemsize for a in arrays)
    return pl.pallas_call(
        kernel,
        out_shape=[jax.ShapeDtypeStruct(s, F32) for s in shapes],
        in_specs=[SMEM] * len(scalars) + [array_spec] * len(arrays),
        out_specs=[VMEM] * len(shapes),
        scratch_shapes=list(scratch),
        compiler_params=pltpu.CompilerParams(vmem_limit_bytes=limit),
        cost_estimate=pl.CostEstimate(flops=flops, bytes_accessed=size, transcendentals=0),
    )(*scalars, *arrays)


def wave_call(sizes, scalars, arrays):
    beams, cols, count, length, tall = sizes
    paired = cols == 2
    deep = 2 * tall + (2 if paired else 4) * length + SUBS
    shapes = [(deep, LANES)] * 2 if paired else [(deep, LANES)] + [(2 * tall, LANES)] * 2
    u = math.gcd(count, TOGETHER)
    return call(
        functools.partial(wave_kernel, beams, cols, count, length),
        shapes,
        scalars,
        arrays + [jnp.asarray(table) for table in dft_blocks(length)],
        [
            pltpu.VMEM((2, 3, tall, LANES), F32),
            pltpu.VMEM((2, 3, tall, LANES), F32),
            pltpu.VMEM((2, 2, length, LANES), F32),
            pltpu.VMEM((SUBS, LANES), F32),
            pltpu.VMEM((u, 2, 2, length, LANES), F32),
            pltpu.VMEM((u, 2 * length, length), BF16),
            pltpu.VMEM((u, length, 2 * length), BF16),
            pltpu.VMEM((u, length, 2 * length), F32),
            pltpu.VMEM((u, 2 * length, length), BF16),
            pltpu.VMEM((u, length, 2 * length), BF16),
            pltpu.VMEM((u, length, 2 * length), F32),
            pltpu.SMEM((2 * count,), jnp.int32),
            pltpu.SemaphoreType.DMA,
        ],
        flops=count * 32 * length**3,
    )


def local(phase_volume, absorb_volume, probe, amplitudes, scan_rows, scan_cols):
    length = probe.shape[1]
    count = scan_rows.shape[2]
    rows_local = phase_volume.shape[1]
    cols_local = phase_volume.shape[2]
    beams, rows, cols = (lax.axis_size(a) for a in ("beam", "row", "col"))
    assert cols_local == LANES and length == 2 * LANES and rows_local == length
    places = jnp.concatenate([scan_rows.reshape(count), scan_cols.reshape(count)])
    part = rows_local // beams
    tall = rows_local + length
    others = range(1, beams)
    near_half = beams // 2

    def swapped(value):
        pairs = []
        for b in range(beams):
            for r in range(rows):
                mate = r ^ 1 if b < near_half else (((r + 1) ^ 1) - 1) % rows
                pairs.append((b * rows + r, b * rows + mate))
        return lax.ppermute(value, ("beam", "row"), pairs)

    beam, row = lax.axis_index("beam"), lax.axis_index("row")
    inside = (beam < near_half) | ((row > 0) & (row < rows - 1))

    sums = call(
        functools.partial(sum_kernel, beams),
        [(2, part, LANES)] * beams,
        [],
        [pltpu.with_memory_space_constraint(x, pltpu.HBM) for x in (phase_volume, absorb_volume)],
        [
            pltpu.VMEM(phase_volume.shape, BF16),
            pltpu.VMEM(phase_volume.shape, BF16),
            pltpu.VMEM((beams, 2, part, LANES), F32),
            pltpu.SemaphoreType.DMA((2 * beams,)),
        ],
        array_spec=HBM,
    )
    sums, amplitudes, probe = lax.optimization_barrier((list(sums), amplitudes, probe))
    total, places = lax.optimization_barrier((collected(sums[0], sums), places))
    near = jnp.where(inside, swapped(total), 0.0)

    def spread(values):
        damping = jnp.exp(-values[1])
        wave = jnp.stack([damping * jnp.cos(values[0]), damping * jnp.sin(values[0])])
        return wave, [wave] + [exchange(wave, "beam", k) for k in others]

    trans, mids = spread(total)
    mids = mids + spread(near)[1]
    if cols == 2:
        lefts = [exchange(x, "col", 1) for x in mids]
        rights = lefts
    else:
        lefts = [lax.ppermute(x, "col", [(i, i + 1) for i in range(cols - 1)]) for x in mids]
        rights = [lax.ppermute(x, "col", [(i + 1, i) for i in range(cols - 1)]) for x in mids]
    paired = cols == 2
    planes = 2 if paired else 4
    outs = wave_call(
        (beams, cols, count, length, tall),
        [],
        [places, *mids, *lefts, *rights, probe, amplitudes.reshape(count, length, length)],
    )
    if paired:
        pieces = [outs[0], exchange(outs[1], "col", 1)]
    else:
        keep, to_left, to_right = outs
        edge = lax.ppermute(to_left, "col", [(i + 1, i) for i in range(cols - 1)])
        edge = edge + lax.ppermute(to_right, "col", [(i, i + 1) for i in range(cols - 1)])
        rest = lax.psum(keep[2 * tall :], "col")
        pieces = [jnp.concatenate([keep[: 2 * tall] + edge, rest])]
    strip = length // beams
    flat = 2 * part + planes * strip + SUBS
    split = call(
        functools.partial(split_kernel, beams, tall, length),
        [(flat, LANES)] * beams + [(2 * part, LANES)] * beams,
        [],
        pieces,
    )

    crossed = swapped(collected(split[beams], split[beams:]))
    summed = collected(split[0], split[:beams])
    whole = summed[: 2 * part] + jnp.where(inside, crossed, 0.0)
    real, imag = whole[:part], whole[part:]
    grad_phase = trans[0] * imag - trans[1] * real
    grad_absorb = -(trans[0] * real + trans[1] * imag)
    squares = grad_phase * grad_phase + grad_absorb * grad_absorb
    squares = squares.reshape(part // SUBS, SUBS, LANES).sum(0)
    gradient = jnp.concatenate([grad_phase, grad_absorb])
    carried = jnp.concatenate([summed[2 * part :], squares])
    carried = butterfly([carried] + [exchange(carried, "row", k) for k in range(1, rows)])
    carried = jnp.concatenate([carried, gradient])
    at = planes * strip + SUBS
    gathered = [carried] + [exchange(carried, "beam", k) for k in others]
    if paired:
        more = [exchange(x[: at + SUBS], "col", 1) for x in gathered]
    else:
        more = [lax.psum(butterfly([x[at : at + SUBS] for x in gathered]), "col")]
    operands = gathered + more
    plane_devices = rows * cols
    objects_step, probe_gradient, loss = call(
        functools.partial(
            final_kernel,
            beams,
            2 if paired else 1,
            planes,
            part,
            1.0 / (2 * rows_local * cols_local * plane_devices),
            float(plane_devices * beams * count),
        ),
        [(2, rows_local, cols_local), (2, length, length), (1, 1)],
        [],
        operands,
    )
    return objects_step, probe_gradient, loss[0, 0]


def solution(mesh):
    in_specs = (
        P("beam", "row", "col"),
        P("beam", "row", "col"),
        P(),
        P("row", "col", "beam", None, None),
        P("row", "col", "beam"),
        P("row", "col", "beam"),
    )
    out_specs = (P(None, "row", "col"), P(), P())
    return jax.shard_map(local, mesh=mesh, in_specs=in_specs, out_specs=out_specs, check_vma=False)
```

```python
import functools
import math

import jax
import jax.numpy as jnp
import numpy as np
from jax import lax
from jax.experimental import pallas as pl
from jax.experimental.pallas import tpu as pltpu
from jax.sharding import PartitionSpec as P

LANES = 128
SUBS = 8
CHUNK = 32
TOGETHER = 8
VMEM = pl.BlockSpec(memory_space=pltpu.VMEM)
SMEM = pl.BlockSpec(memory_space=pltpu.SMEM)
HBM = pl.BlockSpec(memory_space=pltpu.HBM)
F32 = jnp.float32
BF16 = jnp.bfloat16


def dft_blocks(length):
    indices = np.arange(length, dtype=np.int64)
    product = (indices[:, None] * indices[None, :] % length).astype(np.float32)
    angles = (product * np.float32(2.0 * math.pi / length)).astype(np.float64)
    factor = np.float32(1.0 / math.sqrt(length))
    real = (np.cos(angles).astype(np.float32) * factor).astype(jnp.bfloat16)
    imag = (-np.sin(angles).astype(np.float32) * factor).astype(jnp.bfloat16)
    forward = np.block([[real, -imag], [imag, real]])
    backward = np.block([[real, imag], [-imag, real]])
    return forward.astype(jnp.bfloat16), backward.astype(jnp.bfloat16)


def exchange(value, axis, mask):
    count = lax.axis_size(axis)
    return lax.ppermute(value, axis, [(i, i ^ mask) for i in range(count)])


def my_quarter(beams):
    even = 1 - lax.rem(lax.axis_index("row"), 2)
    return jnp.bitwise_xor(lax.axis_index("beam"), even * (beams // 2))


def spots_of(quarter, beams):
    across = jnp.bitwise_xor(quarter, beams // 2)
    return quarter + beams // 2, lax.rem(across + 3 * beams // 2, 2 * beams)


def collected(own, values):
    far_first = {k: exchange(values[k], "beam", k) for k in reversed(range(1, len(values)))}
    return butterfly([own] + [far_first[k] for k in sorted(far_first)])


def butterfly(values):
    while len(values) > 1:
        values = [values[i] + values[i + 1] for i in range(0, len(values), 2)]
    return values[0]


def rows_of(index, size):
    return pl.ds(pl.multiple_of(index * size, size), size)


def sum_kernel(beams, phase_ref, absorb_ref, *refs):
    outs, (phase_now, absorb_now, sums, sems) = refs[:beams], refs[beams:]
    part = phase_now.shape[1] // beams
    copies = []
    for q in range(beams):
        where = pl.ds(q * part, part)
        for comp, (a, b) in enumerate(((phase_ref, phase_now), (absorb_ref, absorb_now))):
            copy = pltpu.make_async_copy(
                a.at[:, where, :], b.at[:, where, :], sems.at[2 * q + comp]
            )
            copy.start()
            copies.append(copy)
    for q in range(beams):
        where = pl.ds(q * part, part)
        for comp, ref in enumerate((phase_now, absorb_now)):
            copies[2 * q + comp].wait()
            total = ref[0, where, :].astype(F32)
            for d in range(1, ref.shape[0]):
                total = total + ref[d, where, :].astype(F32)
            sums[q, comp] = total
    for k in range(beams):
        outs[k][...] = sums[jnp.bitwise_xor(my_quarter(beams), k)]


def wave_kernel(beams, cols, count, length, *refs):
    spot_ref = refs[0]
    held = 2 * beams
    mid_refs, left_refs, right_refs = (refs[1 + i * held : 1 + (i + 1) * held] for i in range(3))
    refs = refs[1 + 3 * held :]
    probe_ref, amp_ref, forward_ref, backward_ref = refs[:4]
    sends = 1 if cols == 2 else 2
    outs = refs[4 : 5 + sends]
    cells, canvas, probe_sum, miss, trans, psi, half_wave, far, chi, back, near = refs[
        5 + sends : -2
    ]
    scan_ref, scan_sem = refs[-2:]
    fetch = pltpu.make_async_copy(spot_ref, scan_ref, scan_sem)
    fetch.start()
    part = mid_refs[0].shape[1]
    tall = cells.shape[2]
    together = trans.shape[0]
    beam, col = my_quarter(beams), lax.axis_index("col")
    has_left, has_right = col > 0, col < cols - 1
    for k in range(beams):
        quarter = jnp.bitwise_xor(beam, k)
        spots = spots_of(quarter, beams)
        for which, at in enumerate(spots):
            where = rows_of(at, part)
            for comp in range(2):
                outside = 1.0 - comp
                source = which * beams + k
                cells[comp, 0, where, :] = jnp.where(has_left, left_refs[source][comp], outside)
                cells[comp, 1, where, :] = mid_refs[source][comp]
                cells[comp, 2, where, :] = jnp.where(has_right, right_refs[source][comp], outside)
    canvas[...] = jnp.zeros_like(canvas)
    probe_sum[...] = jnp.zeros_like(probe_sum)
    miss[...] = jnp.zeros_like(miss)
    lane = lax.broadcasted_iota(jnp.int32, (CHUNK, LANES), 1)
    chunks = length // CHUNK
    fetch.wait()

    def make_psi(s, u):
        row_at, col_at = scan_ref[s], scan_ref[count + s]
        back_shift = lax.rem(LANES - col_at, LANES)
        low = lane < LANES - col_at
        for i in range(chunks):
            here = pl.ds(i * CHUNK, CHUNK)
            there = pl.ds(row_at + i * CHUNK, CHUNK)
            pieces = []
            for comp in range(2):
                turned = [
                    pltpu.roll(cells[comp, j, there, :], back_shift, 1) for j in range(3)
                ]
                pieces.append([jnp.where(low, turned[j], turned[j + 1]) for j in range(2)])
            for j in range(2):
                lanes = pl.ds(j * LANES, LANES)
                real, imag = pieces[0][j], pieces[1][j]
                trans[u, 0, j, here, :] = real
                trans[u, 1, j, here, :] = imag
                probe_real = probe_ref[0, here, lanes]
                probe_imag = probe_ref[1, here, lanes]
                psi[u, here, lanes] = (probe_real * real - probe_imag * imag).astype(BF16)
                psi[u, pl.ds(length + i * CHUNK, CHUNK), lanes] = (
                    probe_real * imag + probe_imag * real
                ).astype(BF16)

    def left_product(table, source, target, u):
        result = jnp.dot(table[...], source[u], preferred_element_type=F32).astype(BF16)
        target[u, :, :length] = result[:length]
        target[u, :, length:] = result[length:]

    def right_product(source, table, target, u):
        for n in range(2):
            lanes = pl.ds(n * length, length)
            target[u, :, lanes] = jnp.dot(
                source[u], table[:, lanes], preferred_element_type=F32
            )

    def make_chi(s, u):
        for i in range(chunks):
            here = pl.ds(i * CHUNK, CHUNK)
            real, imag = far[u, here, :length], far[u, here, length:]
            amplitude = amp_ref[s, here, :].astype(F32)
            power = real * real + imag * imag
            off = jnp.sqrt(power) - amplitude
            wide = off * off
            wide = wide[:, :LANES] + wide[:, LANES:]
            miss[...] += wide.reshape(CHUNK // SUBS, SUBS, LANES).sum(0)
            ratio = 1.0 - amplitude * lax.rsqrt(jnp.maximum(power, 0.25))
            chi[u, here, :] = (real * ratio).astype(BF16)
            chi[u, pl.ds(length + i * CHUNK, CHUNK), :] = (imag * ratio).astype(BF16)

    def scatter(s, u):
        row_at, col_at = scan_ref[s], scan_ref[count + s]
        high = lane >= col_at
        for i in range(chunks):
            here = pl.ds(i * CHUNK, CHUNK)
            there = pl.ds(row_at + i * CHUNK, CHUNK)
            turned = [[], []]
            for j in range(2):
                lanes = pl.ds(j * LANES, LANES)
                grad_real = near[u, here, lanes]
                grad_imag = near[u, here, pl.ds(length + j * LANES, LANES)]
                real, imag = trans[u, 0, j, here, :], trans[u, 1, j, here, :]
                probe_sum[0, j, here, :] += real * grad_real + imag * grad_imag
                probe_sum[1, j, here, :] += real * grad_imag - imag * grad_real
                probe_real = probe_ref[0, here, lanes]
                probe_imag = probe_ref[1, here, lanes]
                turned[0].append(
                    pltpu.roll(probe_real * grad_real + probe_imag * grad_imag, col_at, 1)
                )
                turned[1].append(
                    pltpu.roll(probe_real * grad_imag - probe_imag * grad_real, col_at, 1)
                )
            for comp in range(2):
                first, second = turned[comp]
                canvas[comp, 0, there, :] += jnp.where(high, first, 0.0)
                canvas[comp, 1, there, :] += jnp.where(high, second, first)
                canvas[comp, 2, there, :] += jnp.where(high, 0.0, second)

    def first(s, u):
        make_psi(s, u)
        left_product(forward_ref, psi, half_wave, u)

    def second(s, u):
        right_product(half_wave, backward_ref, far, u)

    def third(s, u):
        make_chi(s, u)
        left_product(backward_ref, chi, back, u)

    def fourth(s, u):
        right_product(back, forward_ref, near, u)

    stages = (first, second, third, fourth, scatter)

    def group(g, carry):
        for t in range(together + len(stages) - 1):
            for k in (1, 4, 3, 2, 0):
                if 0 <= t - k < together:
                    stages[k](g * together + t - k, t - k)
        return carry

    lax.fori_loop(0, count // together, group, 0)
    base = 2 * tall
    if cols == 2:
        tiles = (1, 2 * has_right.astype(jnp.int32))
        comps = ((col,), (1 - col,))
    else:
        tiles = (1, 0, 2)
        comps = ((0, 1), (), ())
    for out, tile, held in zip(outs, tiles, comps):
        for comp in range(2):
            out[pl.ds(comp * tall, tall), :] = canvas[comp, tile]
        for n, comp in enumerate(held):
            for j in range(2):
                out[pl.ds(base + (2 * n + j) * length, length), :] = probe_sum[comp, j]
        if held:
            out[pl.ds(base + 2 * len(held) * length, SUBS), :] = miss[...]


def split_kernel(beams, tall, length, *refs):
    beam = my_quarter(beams)
    ins, outs, edges = refs[: -2 * beams], refs[-2 * beams : -beams], refs[-beams:]
    part = tall // (2 * beams)
    strip = length // beams
    planes = (ins[0].shape[0] - 2 * tall - SUBS) // length

    def fetch(where):
        total = ins[0][where, :]
        for ref in ins[1:]:
            total = total + ref[where, :]
        return total

    for k in range(beams):
        quarter = jnp.bitwise_xor(beam, k)
        spots = spots_of(quarter, beams)
        for out, at in zip((outs[k], edges[k]), spots):
            for comp in range(2):
                where = pl.ds(pl.multiple_of(comp * tall + at * part, SUBS), part)
                out[pl.ds(comp * part, part), :] = fetch(where)
        band = jnp.bitwise_xor(lax.axis_index("beam"), k)
        for n in range(planes):
            start = 2 * tall + n * length + band * strip
            where = pl.ds(pl.multiple_of(start, SUBS), strip)
            outs[k][pl.ds(2 * part + n * strip, strip), :] = fetch(where)
        where = pl.ds(2 * tall + planes * length, SUBS)
        outs[k][pl.ds(2 * part + planes * strip, SUBS), :] = fetch(where)


def final_kernel(beams, halves, planes, part, scale, total, *refs):
    beam, col = my_quarter(beams), lax.axis_index("col")
    gathered = refs[:beams]
    if halves == 2:
        probes = [gathered, refs[beams : 2 * beams]]
    else:
        probes = [gathered]
    object_ref, probe_ref, loss_ref = refs[-3:]
    strip = (gathered[0].shape[0] - 2 * SUBS - 2 * part) // planes
    length = strip * beams
    miss_at = pl.ds(planes * strip, SUBS)
    square_at = pl.ds(planes * strip + SUBS, SUBS)
    for k in range(beams):
        band = jnp.bitwise_xor(lax.axis_index("beam"), k)
        where = rows_of(band, strip)
        for h in range(halves):
            for n in range(planes):
                comp = (jnp.bitwise_xor(col, h)) if halves == 2 else n // 2
                lanes = pl.ds((n % 2) * LANES, LANES)
                probe_ref[comp, where, lanes] = (
                    probes[h][k][pl.ds(n * strip, strip), :] * (1.0 / total)
                )
    if halves == 2:
        squares = butterfly([ref[square_at, :] for ref in probes[0]])
        squares = squares + butterfly([ref[square_at, :] for ref in probes[1]])
    else:
        squares = refs[beams][...]
    mean_square = jnp.sum(squares, keepdims=True) * scale
    factor = jnp.minimum(1.0, 0.5 / jnp.sqrt(mean_square + 1e-06))
    misses = butterfly([ref[miss_at, :] for ref in gathered])
    loss = jnp.sum(misses, keepdims=True) / (beams * total * length * length)
    loss_ref[...] = jnp.broadcast_to(loss, loss_ref.shape)
    base = planes * strip + 2 * SUBS
    for k in range(beams):
        where = rows_of(jnp.bitwise_xor(beam, k), part)
        for comp in range(2):
            object_ref[comp, where, :] = gathered[k][pl.ds(base + comp * part, part), :] * factor


def call(kernel, shapes, scalars, arrays, scratch=(), flops=0, array_spec=VMEM, limit=40 * 2**20):
    size = sum(a.size * a.dtype.itemsize for a in arrays)
    return pl.pallas_call(
        kernel,
        out_shape=[jax.ShapeDtypeStruct(s, F32) for s in shapes],
        in_specs=[SMEM] * len(scalars) + [array_spec] * len(arrays),
        out_specs=[VMEM] * len(shapes),
        scratch_shapes=list(scratch),
        compiler_params=pltpu.CompilerParams(vmem_limit_bytes=limit),
        cost_estimate=pl.CostEstimate(flops=flops, bytes_accessed=size, transcendentals=0),
    )(*scalars, *arrays)


def wave_call(sizes, scalars, arrays):
    beams, cols, count, length, tall = sizes
    paired = cols == 2
    deep = 2 * tall + (2 if paired else 4) * length + SUBS
    shapes = [(deep, LANES)] * 2 if paired else [(deep, LANES)] + [(2 * tall, LANES)] * 2
    u = math.gcd(count, TOGETHER)
    return call(
        functools.partial(wave_kernel, beams, cols, count, length),
        shapes,
        scalars,
        arrays + [jnp.asarray(table) for table in dft_blocks(length)],
        [
            pltpu.VMEM((2, 3, tall, LANES), F32),
            pltpu.VMEM((2, 3, tall, LANES), F32),
            pltpu.VMEM((2, 2, length, LANES), F32),
            pltpu.VMEM((SUBS, LANES), F32),
            pltpu.VMEM((u, 2, 2, length, LANES), F32),
            pltpu.VMEM((u, 2 * length, length), BF16),
            pltpu.VMEM((u, length, 2 * length), BF16),
            pltpu.VMEM((u, length, 2 * length), F32),
            pltpu.VMEM((u, 2 * length, length), BF16),
            pltpu.VMEM((u, length, 2 * length), BF16),
            pltpu.VMEM((u, length, 2 * length), F32),
            pltpu.SMEM((2 * count,), jnp.int32),
            pltpu.SemaphoreType.DMA,
        ],
        flops=count * 32 * length**3,
    )


def local(phase_volume, absorb_volume, probe, amplitudes, scan_rows, scan_cols):
    length = probe.shape[1]
    count = scan_rows.shape[2]
    rows_local = phase_volume.shape[1]
    cols_local = phase_volume.shape[2]
    beams, rows, cols = (lax.axis_size(a) for a in ("beam", "row", "col"))
    assert cols_local == LANES and length == 2 * LANES and rows_local == length
    places = jnp.concatenate([scan_rows.reshape(count), scan_cols.reshape(count)])
    part = rows_local // beams
    tall = rows_local + length
    others = range(1, beams)
    near_half = beams // 2

    def swapped(value):
        pairs = []
        for b in range(beams):
            for r in range(rows):
                mate = r ^ 1 if b < near_half else (((r + 1) ^ 1) - 1) % rows
                pairs.append((b * rows + r, b * rows + mate))
        return lax.ppermute(value, ("beam", "row"), pairs)

    beam, row = lax.axis_index("beam"), lax.axis_index("row")
    inside = (beam < near_half) | ((row > 0) & (row < rows - 1))

    sums = call(
        functools.partial(sum_kernel, beams),
        [(2, part, LANES)] * beams,
        [],
        [pltpu.with_memory_space_constraint(x, pltpu.HBM) for x in (phase_volume, absorb_volume)],
        [
            pltpu.VMEM(phase_volume.shape, BF16),
            pltpu.VMEM(phase_volume.shape, BF16),
            pltpu.VMEM((beams, 2, part, LANES), F32),
            pltpu.SemaphoreType.DMA((2 * beams,)),
        ],
        array_spec=HBM,
    )
    sums, amplitudes, probe = lax.optimization_barrier((list(sums), amplitudes, probe))
    total, places = lax.optimization_barrier((collected(sums[0], sums), places))
    near = jnp.where(inside, swapped(total), 0.0)

    def spread(values):
        damping = jnp.exp(-values[1])
        wave = jnp.stack([damping * jnp.cos(values[0]), damping * jnp.sin(values[0])])
        return wave, [wave] + [exchange(wave, "beam", k) for k in others]

    trans, mids = spread(total)
    mids = mids + spread(near)[1]
    if cols == 2:
        lefts = [exchange(x, "col", 1) for x in mids]
        rights = lefts
    else:
        lefts = [lax.ppermute(x, "col", [(i, i + 1) for i in range(cols - 1)]) for x in mids]
        rights = [lax.ppermute(x, "col", [(i + 1, i) for i in range(cols - 1)]) for x in mids]
    paired = cols == 2
    planes = 2 if paired else 4
    outs = wave_call(
        (beams, cols, count, length, tall),
        [],
        [places, *mids, *lefts, *rights, probe, amplitudes.reshape(count, length, length)],
    )
    if paired:
        pieces = [outs[0], exchange(outs[1], "col", 1)]
    else:
        keep, to_left, to_right = outs
        edge = lax.ppermute(to_left, "col", [(i + 1, i) for i in range(cols - 1)])
        edge = edge + lax.ppermute(to_right, "col", [(i, i + 1) for i in range(cols - 1)])
        rest = lax.psum(keep[2 * tall :], "col")
        pieces = [jnp.concatenate([keep[: 2 * tall] + edge, rest])]
    strip = length // beams
    flat = 2 * part + planes * strip + SUBS
    split = call(
        functools.partial(split_kernel, beams, tall, length),
        [(flat, LANES)] * beams + [(2 * part, LANES)] * beams,
        [],
        pieces,
    )

    crossed = swapped(collected(split[beams], split[beams:]))
    summed = collected(split[0], split[:beams])
    whole = summed[: 2 * part] + jnp.where(inside, crossed, 0.0)
    real, imag = whole[:part], whole[part:]
    grad_phase = trans[0] * imag - trans[1] * real
    grad_absorb = -(trans[0] * real + trans[1] * imag)
    squares = grad_phase * grad_phase + grad_absorb * grad_absorb
    squares = squares.reshape(part // SUBS, SUBS, LANES).sum(0)
    gradient = jnp.concatenate([grad_phase, grad_absorb])
    carried = jnp.concatenate([summed[2 * part :], squares])
    carried = butterfly([carried] + [exchange(carried, "row", k) for k in range(1, rows)])
    carried = jnp.concatenate([carried, gradient])
    at = planes * strip + SUBS
    gathered = [carried] + [exchange(carried, "beam", k) for k in others]
    if paired:
        more = [exchange(x[: at + SUBS], "col", 1) for x in gathered]
    else:
        more = [lax.psum(butterfly([x[at : at + SUBS] for x in gathered]), "col")]
    operands = gathered + more
    plane_devices = rows * cols
    objects_step, probe_gradient, loss = call(
        functools.partial(
            final_kernel,
            beams,
            2 if paired else 1,
            planes,
            part,
            1.0 / (2 * rows_local * cols_local * plane_devices),
            float(plane_devices * beams * count),
        ),
        [(2, rows_local, cols_local), (2, length, length), (1, 1)],
        [],
        operands,
    )
    return objects_step, probe_gradient, loss[0, 0]


def solution(mesh):
    in_specs = (
        P("beam", "row", "col"),
        P("beam", "row", "col"),
        P(),
        P("row", "col", "beam", None, None),
        P("row", "col", "beam"),
        P("row", "col", "beam"),
    )
    out_specs = (P(None, "row", "col"), P(), P())
    return jax.shard_map(local, mesh=mesh, in_specs=in_specs, out_specs=out_specs, check_vma=False)
```
